32 devices in a mesh: dp: 4 (over y, z), tp: 8 (over x, core).
Axes of the slice: x: 4, y: 2, z: 2, core: 2. Of those that a mesh axis runs over, the one named last changes fastest.
The devices are a block of a 4x4x8 slice.
Arguments:
- x: bfloat16 [8, 2048, 2560], P('dp'), parts along dimension 0
- positions: int32 [8, 2048], P('dp'), parts along dimension 0
- lengths: int32 [8], P('dp'), parts along dimension 0
- w_q: bfloat16 [2, 2560, 4096], P(None, None, 'tp')
- w_k: bfloat16 [2, 2560, 1024], P(None, None, 'tp')
- w_v: bfloat16 [2, 2560, 1024], P(None, None, 'tp')
- w_o: bfloat16 [2, 4096, 2560], P(None, 'tp')
- w_gate: bfloat16 [2, 2560, 9728], P(None, None, 'tp')
- w_up: bfloat16 [2, 2560, 9728], P(None, None, 'tp')
- w_down: bfloat16 [2, 9728, 2560], P(None, 'tp')
- norm_gain: float32 [2, 2560], replicated
- q_gain: float32 [2, 32, 128], P(None, 'tp')
- k_gain: float32 [2, 8, 128], P(None, 'tp')
Outputs:
- output 1: bfloat16 [8, 2048, 2560], P('dp'), parts along dimension 0
- output 2: bfloat16 [2, 8, 2048, 8, 128], P(None, 'dp', None, 'tp'), parts along dimension 1
- output 3: bfloat16 [2, 8, 2048, 8, 128], P(None, 'dp', None, 'tp'), parts along dimension 1
There are 4 independent parts. The reference program is written for one: setup_inputs(seed, part) draws one part's arguments, and reference() takes and returns one part's arrays. A program takes and returns all parts, laid end to end along the dimension named above; an argument that names none is the same for every part.
All inputs are finite; a program needn't handle non-finite values.
Results may differ from the reference program's by a relative error of at most 0.0167894.
Values are sent between devices in bfloat16 or wider.
A program may use at most 768 MiB of HBM per device.

```python
import jax
import jax.numpy as jnp
from jax import lax

BATCH_ROWS = 2
SEQ_LEN = 2048
D_MODEL = 2560
N_HEADS = 32
KV_HEADS = 8
KV_SLOTS = 8
FF_WIDTH = 9728
N_LAYERS = 2
HEAD_DIM = 128
POS_OFFSET_RANGE = 8192
ROPE_THETA = 75000000.0
NORM_EPS = 1e-5


def setup_inputs(seed: int = 0, part: int = 0) -> dict:
    part_keys = jax.random.split(jax.random.fold_in(jax.random.key(seed), part), 4)
    shared_keys = jax.random.split(jax.random.key(seed + 1), 10)
    slot_copies = KV_SLOTS // KV_HEADS
    q_width = N_HEADS * HEAD_DIM

    def normal_weight(rng_key, arr_shape, fan_in, factor):
        return (jax.random.normal(rng_key, arr_shape, jnp.float32) * (factor * fan_in ** -0.5)).astype(jnp.bfloat16)

    def slot_weight(rng_key):
        head_draw = jax.random.normal(rng_key, (N_LAYERS, D_MODEL, KV_HEADS, HEAD_DIM), jnp.float32) * D_MODEL ** -0.5
        return jnp.repeat(head_draw, slot_copies, axis=2).reshape(N_LAYERS, D_MODEL, KV_SLOTS * HEAD_DIM).astype(jnp.bfloat16)

    def gain_draw(rng_key, arr_shape):
        return 1.0 + 0.3 * jax.random.normal(rng_key, arr_shape, jnp.float32)

    x = jax.random.normal(part_keys[0], (BATCH_ROWS, SEQ_LEN, D_MODEL), jnp.float32).astype(jnp.bfloat16)
    offsets = jax.random.randint(part_keys[1], (BATCH_ROWS,), 0, POS_OFFSET_RANGE, jnp.int32)
    positions = offsets[:, None] + jnp.arange(SEQ_LEN, dtype=jnp.int32)[None, :]
    drawn_lengths = jax.random.randint(part_keys[2], (BATCH_ROWS,), 1, SEQ_LEN + 1, jnp.int32)
    full_row = jax.random.randint(part_keys[3], (), 0, BATCH_ROWS, jnp.int32)
    lengths = jnp.where(jnp.arange(BATCH_ROWS, dtype=jnp.int32) == full_row, SEQ_LEN, drawn_lengths).astype(jnp.int32)
    out_factor = 2.0 * SEQ_LEN ** 0.125
    k_gain = jnp.repeat(gain_draw(shared_keys[9], (N_LAYERS, KV_HEADS, HEAD_DIM)), slot_copies, axis=1)
    return {
        'x': x,
        'positions': positions,
        'lengths': lengths,
        'w_q': normal_weight(shared_keys[0], (N_LAYERS, D_MODEL, q_width), D_MODEL, 1.0),
        'w_k': slot_weight(shared_keys[1]),
        'w_v': slot_weight(shared_keys[2]),
        'w_o': normal_weight(shared_keys[3], (N_LAYERS, q_width, D_MODEL), q_width, out_factor),
        'w_gate': normal_weight(shared_keys[4], (N_LAYERS, D_MODEL, FF_WIDTH), D_MODEL, 1.0),
        'w_up': normal_weight(shared_keys[5], (N_LAYERS, D_MODEL, FF_WIDTH), D_MODEL, 1.0),
        'w_down': normal_weight(shared_keys[6], (N_LAYERS, FF_WIDTH, D_MODEL), FF_WIDTH, 1.0),
        'norm_gain': gain_draw(shared_keys[7], (N_LAYERS, D_MODEL)),
        'q_gain': gain_draw(shared_keys[8], (N_LAYERS, N_HEADS, HEAD_DIM)),
        'k_gain': k_gain,
    }


def norm_rows(values, gain_vec):
    as_float = values.astype(jnp.float32)
    row_mean = jnp.mean(as_float, axis=-1, keepdims=True)
    centered = as_float - row_mean
    variance = jnp.mean(centered * centered, axis=-1, keepdims=True)
    return centered * lax.rsqrt(variance + NORM_EPS) * gain_vec


def apply_rope(values, cos_table, sin_table):
    pairs = values.reshape(values.shape[:-1] + (HEAD_DIM // 2, 2))
    even_part = pairs[..., 0]
    odd_part = pairs[..., 1]
    rotated = jnp.stack([even_part * cos_table - odd_part * sin_table, odd_part * cos_table + even_part * sin_table], axis=-1)
    return rotated.reshape(values.shape)


def reference(x, positions, lengths, w_q, w_k, w_v, w_o, w_gate, w_up, w_down, norm_gain, q_gain, k_gain):
    exponents = jnp.arange(HEAD_DIM // 2, dtype=jnp.float32) * (2.0 / HEAD_DIM)
    angles = positions.astype(jnp.float32)[:, :, None] * ROPE_THETA ** (-exponents)
    cos_table = jnp.cos(angles)[:, :, None, :]
    sin_table = jnp.sin(angles)[:, :, None, :]
    token_count = BATCH_ROWS * SEQ_LEN
    group_size = N_HEADS // KV_SLOTS
    seq_index = jnp.arange(SEQ_LEN)
    causal = seq_index[None, :] <= seq_index[:, None]
    score_scale = HEAD_DIM ** -0.5

    def attend_row(row_inputs):
        q_row, k_row, v_row, row_len = row_inputs
        allowed = causal & (seq_index[None, :] < row_len)
        q_first = jnp.transpose(q_row, (1, 0, 2))

        def one_head(head_idx):
            q_head = lax.dynamic_index_in_dim(q_first, head_idx, 0, keepdims=False)
            slot_idx = head_idx // group_size
            k_head = lax.dynamic_index_in_dim(k_row, slot_idx, 1, keepdims=False)
            v_head = lax.dynamic_index_in_dim(v_row, slot_idx, 1, keepdims=False)
            scores = jnp.dot(q_head, k_head.T, preferred_element_type=jnp.float32) * score_scale
            scores = jnp.where(allowed, scores, -1e30)
            attn_probs = jax.nn.softmax(scores, axis=-1).astype(jnp.bfloat16)
            return jnp.dot(attn_probs, v_head, preferred_element_type=jnp.float32).astype(jnp.bfloat16)

        head_outs = lax.map(one_head, jnp.arange(N_HEADS))
        return jnp.transpose(head_outs, (1, 0, 2)).reshape(SEQ_LEN, N_HEADS * HEAD_DIM)

    def layer_step(hidden, layer_weights):
        q_weight, k_weight, v_weight, o_weight, gate_weight, up_weight, down_weight, ln_gain, qn_gain, kn_gain = layer_weights
        normed = norm_rows(hidden, ln_gain).astype(jnp.bfloat16).reshape(token_count, D_MODEL)
        q_proj = jnp.dot(normed, q_weight, preferred_element_type=jnp.float32).reshape(BATCH_ROWS, SEQ_LEN, N_HEADS, HEAD_DIM)
        k_proj = jnp.dot(normed, k_weight, preferred_element_type=jnp.float32).reshape(BATCH_ROWS, SEQ_LEN, KV_SLOTS, HEAD_DIM)
        v_proj = jnp.dot(normed, v_weight, preferred_element_type=jnp.float32).astype(jnp.bfloat16).reshape(BATCH_ROWS, SEQ_LEN, KV_SLOTS, HEAD_DIM)
        q_rot = apply_rope(norm_rows(q_proj, qn_gain), cos_table, sin_table).astype(jnp.bfloat16)
        k_rot = apply_rope(norm_rows(k_proj, kn_gain), cos_table, sin_table).astype(jnp.bfloat16)
        attn_out = lax.map(attend_row, (q_rot, k_rot, v_proj, lengths)).reshape(token_count, N_HEADS * HEAD_DIM)
        gate_proj = jnp.dot(normed, gate_weight, preferred_element_type=jnp.float32)
        up_proj = jnp.dot(normed, up_weight, preferred_element_type=jnp.float32)
        mlp_act = (jax.nn.silu(gate_proj) * up_proj).astype(jnp.bfloat16)
        branch_sum = jnp.dot(attn_out, o_weight, preferred_element_type=jnp.float32) + jnp.dot(mlp_act, down_weight, preferred_element_type=jnp.float32)
        new_hidden = (hidden.reshape(token_count, D_MODEL).astype(jnp.float32) + branch_sum).astype(jnp.bfloat16)
        return new_hidden.reshape(BATCH_ROWS, SEQ_LEN, D_MODEL), (k_rot, v_proj)

    y, caches = lax.scan(layer_step, x, (w_q, w_k, w_v, w_o, w_gate, w_up, w_down, norm_gain, q_gain, k_gain))
    return y, caches[0], caches[1]
```

```python
import functools

import jax
import jax.numpy as jnp
from jax import lax
from jax.experimental import pallas as pl
from jax.experimental.pallas import tpu as pltpu
from jax.sharding import PartitionSpec as P

HEAD_DIM = 128
ROPE_THETA = 75000000.0
NORM_EPS = 1e-5
NEG = -1e30
LOG2E = 1.4426950408889634
CHUNK_ROWS = 512
MESH = pl.DeviceIdType.MESH
F32 = jnp.float32
BF16 = jnp.bfloat16

SIB, M1L, M1R, M2L, M2R, M3L, M3R, A1L, A1R, A2L, A2R, A3L, A3R, AS = range(14)
N_MSG = 14


def mm(a, b):
    return jnp.dot(a, b, preferred_element_type=F32)


def norm_last(values, gain):
    width = values.shape[-1]
    mean = jnp.sum(values, axis=-1, keepdims=True) * (1.0 / width)
    centered = values - mean
    var = jnp.sum(centered * centered, axis=-1, keepdims=True) * (1.0 / width)
    return centered * lax.rsqrt(var + NORM_EPS) * gain


def rope(values, cos, sin):
    lane = lax.broadcasted_iota(jnp.int32, values.shape, 1)
    swapped = jnp.where(lane % 2 == 0, pltpu.roll(values, HEAD_DIM - 1, 1), pltpu.roll(values, 1, 1))
    return values * cos + swapped * sin


def layers_kernel(
    cfg,
    len_ref, x_ref, cos_ref, sin_ref, wq_ref, wk_ref, wv_ref, wo_ref, wg_ref, wu_ref, wd_ref, ng_ref, qg_ref, kg_ref,
    out_ref, kc_ref, vc_ref,
    wqkv, wg, wu, wod, xn, cs, sn, act, q_scr, k_scr, v_scr, m_scr, acc_scr, part, rsib, own, ro, rf, ag, hres,
    w_sem, in_sem, kv_sem, res_sem, ago_sem, s_sem, r_sem,
):
    n_layers, n_chunks, rows, per_seq, heads, chips = cfg
    width = x_ref.shape[1]
    half = width // 2
    ff = wg_ref.shape[2]
    qw = heads * HEAD_DIM
    quarter = rows // (2 * chips)
    hrows = rows // 2
    total = n_layers * n_chunks
    c_exp = HEAD_DIM ** -0.5 * LOG2E

    me = lax.axis_index("tp")
    chip, core = me // 2, me % 2
    left_chip, right_chip, far_chip = (chip + chips - 1) % chips, (chip + 1) % chips, (chip + 2) % chips
    left, right, sib = left_chip * 2 + core, right_chip * 2 + core, chip * 2 + 1 - core
    my_base, sib_base = core * hrows, (1 - core) * hrows

    def block(chip_id):
        return pl.ds(pl.multiple_of(my_base + chip_id * quarter, quarter), quarter)

    def sub(chip_id):
        return pl.ds(pl.multiple_of(chip_id * quarter, quarter), quarter)

    my_half = pl.ds(pl.multiple_of(my_base, hrows), hrows)
    sib_half = pl.ds(pl.multiple_of(sib_base, hrows), hrows)
    first, second = pl.ds(0, half), pl.ds(half, half)

    def msg(kind, slot, src, dst, dev):
        return pltpu.make_async_remote_copy(
            src_ref=src, dst_ref=dst, send_sem=s_sem.at[kind, slot], recv_sem=r_sem.at[kind, slot],
            device_id={"tp": dev}, device_id_type=MESH,
        )

    def messages(slot):
        p, a = part.at[slot], ag.at[slot]
        mine, lb, rb, fb = block(chip), block(left_chip), block(right_chip), block(far_chip)
        table = {
            SIB: (p.at[sib_half], rsib.at[slot], sib),
            M1L: (p.at[fb, first], ro.at[slot, 0], left),
            M1R: (p.at[fb, second], ro.at[slot, 1], right),
            M2L: (p.at[lb, second], rf.at[slot, 0, :, second], left),
            M2R: (p.at[rb, first], rf.at[slot, 1, :, first], right),
            M3L: (p.at[lb, first], rf.at[slot, 0, :, first], left),
            M3R: (p.at[rb, second], rf.at[slot, 1, :, second], right),
            A1L: (a.at[mine, first], a.at[mine, first], left),
            A1R: (a.at[mine, second], a.at[mine, second], right),
            A2L: (a.at[mine, second], a.at[mine, second], left),
            A2R: (a.at[mine, first], a.at[mine, first], right),
            A3L: (a.at[rb, first], a.at[rb, first], left),
            A3R: (a.at[lb, second], a.at[lb, second], right),
            AS: (a.at[my_half], a.at[my_half], sib),
        }
        return lambda kind: msg(kind, slot, *table[kind])

    def chunk_rows(g):
        return pl.ds(pl.multiple_of((g % n_chunks) * rows, rows), rows)

    def weight_copies(which, layer):
        groups = {
            "qkv": [
                (wq_ref.at[layer], wqkv.at[:, pl.ds(0, qw)], 0),
                (wk_ref.at[layer], wqkv.at[:, pl.ds(qw, HEAD_DIM)], 1),
                (wv_ref.at[layer], wqkv.at[:, pl.ds(qw + HEAD_DIM, HEAD_DIM)], 2),
            ],
            "ff": [(wg_ref.at[layer], wg, 3), (wu_ref.at[layer], wu, 4)],
            "od": [(wo_ref.at[layer], wod.at[pl.ds(0, qw)], 5), (wd_ref.at[layer], wod.at[pl.ds(qw, ff)], 6)],
        }
        return [pltpu.make_async_copy(src, dst, w_sem.at[n]) for src, dst, n in groups[which]]

    def start_input(g, slot):
        r = chunk_rows(g)

        @pl.when(g < n_chunks)
        def _():
            pltpu.make_async_copy(x_ref.at[r], xn.at[slot], in_sem.at[0, slot]).start()

        @pl.when(g >= n_chunks)
        def _():
            pltpu.make_async_copy(out_ref.at[g // n_chunks - 1, r], xn.at[slot], in_sem.at[0, slot]).start()

        pltpu.make_async_copy(cos_ref.at[r], cs.at[slot], in_sem.at[1, slot]).start()
        pltpu.make_async_copy(sin_ref.at[r], sn.at[slot], in_sem.at[2, slot]).start()

    def wait_input(g, slot):
        r = chunk_rows(g)
        pltpu.make_async_copy(x_ref.at[r], xn.at[slot], in_sem.at[0, slot]).wait()
        pltpu.make_async_copy(cos_ref.at[r], cs.at[slot], in_sem.at[1, slot]).wait()
        pltpu.make_async_copy(sin_ref.at[r], sn.at[slot], in_sem.at[2, slot]).wait()

    def seq_start(g):
        return pl.multiple_of((g % per_seq) * rows, rows)

    def kv_copies(g):
        here = pl.ds(seq_start(g), rows)
        r = chunk_rows(g)
        return [
            pltpu.make_async_copy(k_scr.at[here, pl.ds(0, HEAD_DIM)], kc_ref.at[g // n_chunks, r], kv_sem.at[0]),
            pltpu.make_async_copy(v_scr.at[here, pl.ds(0, HEAD_DIM)], vc_ref.at[g // n_chunks, r], kv_sem.at[1]),
        ]

    def ag_out(g, slot, base, n):
        dst = pl.ds(pl.multiple_of((g % n_chunks) * rows + base, hrows), hrows)
        src = pl.ds(pl.multiple_of(base, hrows), hrows)
        return pltpu.make_async_copy(ag.at[slot, src], out_ref.at[g // n_chunks, dst], ago_sem.at[n, slot])

    def residual_copy(c):
        src = pl.ds(pl.multiple_of(c * rows + my_base + chip * quarter, quarter), quarter)
        return pltpu.make_async_copy(x_ref.at[src], hres.at[c], res_sem.at[c])

    def reduce_first(g):
        slot = g % 2
        m = messages(slot)
        m(SIB).wait_recv()
        p, s = part.at[slot], rsib.at[slot]

        def fold(chip_id):
            b = block(chip_id)
            p[b, :] = (p[b, :].astype(F32) + s[sub(chip_id), :].astype(F32)).astype(BF16)

        fold(far_chip)
        m(M1L).start()
        m(M1R).start()
        fold(left_chip)
        m(M2L).start()
        fold(right_chip)
        m(M2R).start()
        own[...] = p[block(chip), :].astype(F32) + s[sub(chip), :].astype(F32)

    def reduce_second(g):
        slot = g % 2
        m = messages(slot)
        p = part.at[slot]
        m(M1L).wait_recv()
        lb, rb = block(left_chip), block(right_chip)
        p[lb, first] = (p[lb, first].astype(F32) + ro[slot, 0].astype(F32)).astype(BF16)
        m(M3L).start()
        m(M1R).wait_recv()
        p[rb, second] = (p[rb, second].astype(F32) + ro[slot, 1].astype(F32)).astype(BF16)
        m(M3R).start()

    def reduce_last(g):
        slot = g % 2
        c = g % n_chunks
        m = messages(slot)
        for kind in (M2L, M2R, M3L, M3R):
            m(kind).wait_recv()

        @pl.when(g < n_chunks)
        def _():
            residual_copy(c).wait()

        h = (own[...] + (rf[slot, 0].astype(F32) + rf[slot, 1].astype(F32)) + hres[c].astype(F32)).astype(BF16)
        mine = block(chip)

        @pl.when(g < total - n_chunks)
        def _():
            hres[c] = h
            gain = ng_ref[pl.ds(g // n_chunks + 1, 1), :]
            ag[slot, mine, :] = norm_last(h.astype(F32), gain).astype(BF16)

        @pl.when(g >= total - n_chunks)
        def _():
            ag[slot, mine, :] = h

        for kind in (A1L, A1R, A2L, A2R):
            m(kind).start()

    def gather_forward(g):
        m = messages(g % 2)
        m(A1L).wait_recv()
        m(A3L).start()
        m(A1R).wait_recv()
        m(A3R).start()

    def gather_last(g):
        slot = g % 2
        m = messages(slot)
        for kind in (A2L, A2R, A3L, A3R):
            m(kind).wait_recv()
        m(AS).start()
        ag_out(g, slot, my_base, 0).start()

    def gather_sibling(g):
        slot = g % 2
        messages(slot)(AS).wait_recv()
        ag_out(g, slot, sib_base, 1).start()

    def gather_done(g):
        slot = g % 2
        m = messages(slot)
        for kind in (A1L, A1R, A2L, A2R, A3L, A3R, AS):
            m(kind).wait_send()
        ag_out(g, slot, my_base, 0).wait()
        ag_out(g, slot, sib_base, 1).wait()

    def reduce_done(g):
        m = messages(g % 2)
        for kind in (SIB, M1L, M1R, M2L, M2R, M3L, M3R):
            m(kind).wait_send()

    def guarded(g, fn):
        @pl.when(jnp.logical_and(g >= 0, g < total))
        def _():
            fn(g)

    def load_chunk(g):
        slot = g % 2
        wait_input(g, slot)

        @pl.when(g + 1 < total)
        def _():
            start_input(g + 1, (g + 1) % 2)

        @pl.when(g < n_chunks)
        def _():
            step = 128 if rows % 128 == 0 else rows

            def body(r, carry):
                rr = pl.ds(pl.multiple_of(r * step, step), step)
                xn[slot, rr, :] = norm_last(xn[slot, rr, :].astype(F32), ng_ref[0:1, :]).astype(BF16)
                return carry

            lax.fori_loop(0, rows // step, body, 0)

    def head(values, gain, slot):
        return rope(norm_last(values, gain), cs[slot], sn[slot]).astype(BF16)

    def projections(g):
        slot = g % 2
        layer = g // n_chunks
        here = pl.ds(seq_start(g), rows)
        n = xn[slot]
        z = mm(n, wqkv[:, qw:qw + 2 * HEAD_DIM])
        k_scr[here, :HEAD_DIM] = head(z[:, :HEAD_DIM], kg_ref[layer], slot)
        v_scr[here, :HEAD_DIM] = z[:, HEAD_DIM:].astype(BF16)
        pos = seq_start(g) + lax.broadcasted_iota(jnp.int32, (rows, HEAD_DIM), 0)
        lane = lax.broadcasted_iota(jnp.int32, (rows, HEAD_DIM), 1)
        length = len_ref[(g % n_chunks) // per_seq]
        k_scr[here, HEAD_DIM:] = jnp.where(jnp.logical_and(lane == 0, pos >= length), NEG, 0.0).astype(BF16)
        for pair in range(heads // 2):
            z = mm(n, wqkv[:, pair * 2 * HEAD_DIM:(pair + 1) * 2 * HEAD_DIM])
            for e in range(2):
                hd = 2 * pair + e
                q_scr[hd, :, :HEAD_DIM] = head(z[:, e * HEAD_DIM:(e + 1) * HEAD_DIM], qg_ref[layer, hd:hd + 1, :], slot)

    def attention(g):
        s0 = seq_start(g)

        def scores(hd, keys):
            return lax.dot_general(q_scr[hd], k_scr[keys, :], (((1,), (1,)), ((), ())), preferred_element_type=F32)

        keys = pl.ds(s0, rows)
        causal = lax.broadcasted_iota(jnp.int32, (rows, rows), 1) <= lax.broadcasted_iota(jnp.int32, (rows, rows), 0)
        for hd in range(heads):
            s = jnp.where(causal, scores(hd, keys), NEG)
            top = jnp.max(s, axis=-1, keepdims=True)
            p = jnp.exp2((s - top) * c_exp).astype(BF16)
            m_scr[hd] = jnp.broadcast_to(top, (rows, HEAD_DIM))
            acc_scr[hd] = mm(p, v_scr[keys, :])

        def body(j, carry):
            keys = pl.ds(pl.multiple_of(j * rows, rows), rows)
            for hd in range(heads):
                s = scores(hd, keys)
                old = m_scr[hd, :, 0:1]
                top = jnp.maximum(old, jnp.max(s, axis=-1, keepdims=True))
                p = jnp.exp2((s - top) * c_exp).astype(BF16)
                scale = jnp.exp2((old - top) * c_exp)
                m_scr[hd] = jnp.broadcast_to(top, (rows, HEAD_DIM))
                acc_scr[hd] = acc_scr[hd] * scale + mm(p, v_scr[keys, :])
            return carry

        lax.fori_loop(0, g % per_seq, body, 0)
        for hd in range(heads):
            out = acc_scr[hd, :, :HEAD_DIM] / acc_scr[hd, :, HEAD_DIM:]
            act[:, hd * HEAD_DIM:(hd + 1) * HEAD_DIM] = out.astype(BF16)

    def feed_forward(g):
        n = xn[g % 2]
        for c0 in range(0, ff, 256):
            c1 = min(c0 + 256, ff)
            gate = mm(n, wg[:, c0:c1])
            up = mm(n, wu[:, c0:c1])
            act[:, qw + c0:qw + c1] = (jax.nn.silu(gate) * up).astype(BF16)

    def output(g):
        p = part.at[g % 2]
        step = 512 if width % 512 == 0 else width
        for c0 in range(0, width, step):
            p[:, c0:c0 + step] = mm(act[...], wod[:, c0:c0 + step]).astype(BF16)

    def layer_start(g, which):
        @pl.when(g % n_chunks == 0)
        def _():
            for copy in weight_copies(which, g // n_chunks):
                copy.wait()

    def layer_end(g, which):
        @pl.when(jnp.logical_and(g % n_chunks == n_chunks - 1, g < total - 1))
        def _():
            for copy in weight_copies(which, g // n_chunks + 1):
                copy.start()

    barrier = pltpu.get_barrier_semaphore()
    for dev in (left, right, sib):
        pl.semaphore_signal(barrier, inc=1, device_id={"tp": dev}, device_id_type=MESH)
    pl.semaphore_wait(barrier, 3)

    start_input(0, 0)
    for which in ("qkv", "ff", "od"):
        for copy in weight_copies(which, 0):
            copy.start()
    for c in range(n_chunks):
        residual_copy(c).start()
    q_scr[:, :, HEAD_DIM:] = jnp.ones((heads, rows, HEAD_DIM), BF16)
    v_scr[:, HEAD_DIM:] = jnp.ones((v_scr.shape[0], HEAD_DIM), BF16)
    pad = act.shape[1] - (qw + ff)
    if pad:
        act[:, qw + ff:] = jnp.zeros((rows, pad), BF16)
        wod[qw + ff:, :] = jnp.zeros((pad, width), BF16)

    def step(i, carry):
        busy = i < total

        @pl.when(busy)
        def _():
            load_chunk(i)
            layer_start(i, "qkv")
            projections(i)
            layer_end(i, "qkv")
            for copy in kv_copies(i):
                copy.start()
            attention(i)
            for copy in kv_copies(i):
                copy.wait()

        guarded(i - 2, reduce_done)
        guarded(i - 3, gather_sibling)
        guarded(i - 1, reduce_first)

        @pl.when(busy)
        def _():
            layer_start(i, "ff")
            feed_forward(i)
            layer_end(i, "ff")

        guarded(i - 3, gather_done)
        guarded(i - 1, reduce_second)
        guarded(i - 2, gather_forward)

        @pl.when(busy)
        def _():
            layer_start(i, "od")
            output(i)
            layer_end(i, "od")
            messages(i % 2)(SIB).start()

        guarded(i - 1, reduce_last)
        guarded(i - 2, gather_last)
        return carry

    lax.fori_loop(0, total + 3, step, 0)


def run_layers(x, cos, sin, lengths, w_q, w_k, w_v, w_o, w_gate, w_up, w_down, norm_gain, q_gain, k_gain, n_tp):
    n_batch, seq, width = x.shape
    n_layers = w_q.shape[0]
    heads = w_q.shape[2] // HEAD_DIM
    ff = w_gate.shape[2]
    rows = min(CHUNK_ROWS, seq // 4)
    tokens = n_batch * seq
    n_chunks, per_seq, chips = tokens // rows, seq // rows, n_tp // 2
    quarter = rows // n_tp
    act_width = -(-(heads * HEAD_DIM + ff) // 256) * 256
    cfg = (n_layers, n_chunks, rows, per_seq, heads, chips)
    any_spec = pl.BlockSpec(memory_space=pl.ANY)
    vmem_spec = pl.BlockSpec(memory_space=pltpu.VMEM)
    dma = pltpu.SemaphoreType.DMA
    out, kc, vc = pl.pallas_call(
        functools.partial(layers_kernel, cfg),
        name="layers",
        out_shape=(
            jax.ShapeDtypeStruct((n_layers, tokens, width), BF16),
            jax.ShapeDtypeStruct((n_layers, tokens, HEAD_DIM), BF16),
            jax.ShapeDtypeStruct((n_layers, tokens, HEAD_DIM), BF16),
        ),
        in_specs=[pl.BlockSpec(memory_space=pltpu.SMEM)] + [any_spec] * 10 + [vmem_spec] * 3,
        out_specs=(any_spec, any_spec, any_spec),
        scratch_shapes=[
            pltpu.VMEM((width, (heads + 2) * HEAD_DIM), BF16),
            pltpu.VMEM((width, ff), BF16),
            pltpu.VMEM((width, ff), BF16),
            pltpu.VMEM((act_width, width), BF16),
            pltpu.VMEM((2, rows, width), BF16),
            pltpu.VMEM((2, rows, HEAD_DIM), F32),
            pltpu.VMEM((2, rows, HEAD_DIM), F32),
            pltpu.VMEM((rows, act_width), BF16),
            pltpu.VMEM((heads, rows, 2 * HEAD_DIM), BF16),
            pltpu.VMEM((seq, 2 * HEAD_DIM), BF16),
            pltpu.VMEM((seq, 2 * HEAD_DIM), BF16),
            pltpu.VMEM((heads, rows, HEAD_DIM), F32),
            pltpu.VMEM((heads, rows, 2 * HEAD_DIM), F32),
            pltpu.VMEM((2, rows, width), BF16),
            pltpu.VMEM((2, rows // 2, width), BF16),
            pltpu.VMEM((quarter, width), F32),
            pltpu.VMEM((2, 2, quarter, width // 2), BF16),
            pltpu.VMEM((2, 2, quarter, width), BF16),
            pltpu.VMEM((2, rows, width), BF16),
            pltpu.VMEM((n_chunks, quarter, width), BF16),
            dma((7,)), dma((3, 2)), dma((2,)), dma((n_chunks,)), dma((2, 2)), dma((N_MSG, 2)), dma((N_MSG, 2)),
        ],
        compiler_params=pltpu.CompilerParams(collective_id=0, has_side_effects=True, vmem_limit_bytes=67043328),
    )(
        lengths, x.reshape(tokens, width), cos, sin, w_q, w_k, w_v, w_o, w_gate, w_up, w_down, norm_gain, q_gain, k_gain
    )
    y = out[n_layers - 1].reshape(n_batch, seq, width)
    cache_shape = (n_layers, n_batch, seq, 1, HEAD_DIM)
    return y, kc.reshape(cache_shape), vc.reshape(cache_shape)


def rope_tables(positions):
    lane = jnp.arange(HEAD_DIM)
    exponents = (lane // 2).astype(F32) * (2.0 / HEAD_DIM)
    angles = positions.reshape(-1).astype(F32)[:, None] * ROPE_THETA ** (-exponents)
    sign = jnp.where(lane % 2 == 0, -1.0, 1.0).astype(F32)
    return jnp.cos(angles), jnp.sin(angles) * sign


def solution(mesh):
    act_spec = P('dp', None, None)
    col_spec = P(None, None, 'tp')
    row_spec = P(None, 'tp', None)
    cache_spec = P(None, 'dp', None, 'tp', None)
    in_specs = (act_spec, P('dp', None), P('dp'), col_spec, col_spec, col_spec, row_spec, col_spec, col_spec, row_spec, P(None, None), row_spec, row_spec)
    n_tp = mesh.shape['tp']

    def device_body(x, positions, lengths, w_q, w_k, w_v, w_o, w_gate, w_up, w_down, norm_gain, q_gain, k_gain):
        cos, sin = rope_tables(positions)
        return run_layers(x, cos, sin, lengths, w_q, w_k, w_v, w_o, w_gate, w_up, w_down, norm_gain, q_gain, k_gain, n_tp)

    return jax.shard_map(device_body, mesh=mesh, in_specs=in_specs, out_specs=(act_spec, cache_spec, cache_spec), check_vma=False)
```

```python
import functools

import jax
import jax.numpy as jnp
from jax import lax
from jax.experimental import pallas as pl
from jax.experimental.pallas import tpu as pltpu
from jax.sharding import PartitionSpec as P

HEAD_DIM = 128
ROPE_THETA = 75000000.0
NORM_EPS = 1e-5
NEG = -1e30
LOG2E = 1.4426950408889634
CHUNK_ROWS = 512
AG_SLOTS = 3
MESH = pl.DeviceIdType.MESH
F32 = jnp.float32
BF16 = jnp.bfloat16

SIB, M1L, M1R, M2L, M2R, M3L, M3R, A1L, A1R, A2L, A2R, A3L, A3R, AS = range(14)
N_MSG = 14


def mm(a, b):
    return jnp.dot(a, b, preferred_element_type=F32)


def mm_t(a, b):
    return lax.dot_general(a, b, (((1,), (1,)), ((), ())), preferred_element_type=F32)


def norm_last(values, gain):
    width = values.shape[-1]
    mean = jnp.sum(values, axis=-1, keepdims=True) * (1.0 / width)
    centered = values - mean
    var = jnp.sum(centered * centered, axis=-1, keepdims=True) * (1.0 / width)
    return centered * lax.rsqrt(var + NORM_EPS) * gain


def cos_sin(angles):
    turns = jnp.round(angles * 0.6366197723675814)
    r = ((angles - turns * 1.5703125) - turns * 4.837512969970703e-4) - turns * 7.549789954891882e-8
    r2 = r * r
    sin_r = r + r * r2 * (-1.6666654611e-1 + r2 * (8.3321608736e-3 - r2 * 1.9515295891e-4))
    cos_r = 1.0 - 0.5 * r2 + r2 * r2 * (4.166664568298827e-2 + r2 * (-1.388731625493765e-3 + r2 * 2.443315711809948e-5))
    quad = turns.astype(jnp.int32) & 3
    odd = (quad & 1) == 1
    cos = jnp.where(odd, sin_r, cos_r)
    sin = jnp.where(odd, cos_r, sin_r)
    cos = jnp.where((quad == 1) | (quad == 2), -cos, cos)
    sin = jnp.where(quad >= 2, -sin, sin)
    return cos, sin


def rope(values, cos, sin):
    lane = lax.broadcasted_iota(jnp.int32, values.shape, 1)
    swapped = jnp.where(lane % 2 == 0, pltpu.roll(values, HEAD_DIM - 1, 1), pltpu.roll(values, 1, 1))
    return values * cos + swapped * sin


def layers_kernel(
    cfg,
    len_ref, x_ref, pos_ref, wq_ref, wk_ref, wv_ref, wo_ref, wg_ref, wu_ref, wd_ref, ng_ref, qg_ref, kg_ref, fr_ref,
    h_ref, y_ref, kc_ref, vc_ref,
    wqkv, wg, wu, wod, xn, pos, cs, sn, act, q_scr, k_scr, v_scr, m_scr, acc_scr, part, rsib, m3, own, ro, rf, ag, hres,
    w_sem, in_sem, kv_sem, res_sem, ago_sem, s_sem, r_sem, credit,
):
    n_layers, n_chunks, rows, per_seq, heads, chips = cfg
    width = x_ref.shape[1]
    half = width // 2
    ff = wg_ref.shape[1]
    qw = heads * HEAD_DIM
    quarter = rows // (2 * chips)
    hrows = rows // 2
    total = n_layers * n_chunks
    c_exp = HEAD_DIM ** -0.5 * LOG2E

    me = lax.axis_index("tp")
    chip, core = me // 2, me % 2
    left_chip, right_chip, far_chip = (chip + chips - 1) % chips, (chip + 1) % chips, (chip + 2) % chips
    left, right, sib = left_chip * 2 + core, right_chip * 2 + core, chip * 2 + 1 - core
    my_base, sib_base = core * hrows, (1 - core) * hrows

    def block(chip_id):
        return pl.ds(pl.multiple_of(my_base + chip_id * quarter, quarter), quarter)

    def sub(chip_id):
        return pl.ds(pl.multiple_of(chip_id * quarter, quarter), quarter)

    my_half = pl.ds(pl.multiple_of(my_base, hrows), hrows)
    sib_half = pl.ds(pl.multiple_of(sib_base, hrows), hrows)
    first, second = pl.ds(0, half), pl.ds(half, half)

    def msg(kind, slot, src, dst, dev):
        return pltpu.make_async_remote_copy(
            src_ref=src, dst_ref=dst, send_sem=s_sem.at[kind, slot], recv_sem=r_sem.at[kind, slot],
            device_id={"tp": dev}, device_id_type=MESH,
        )

    def messages(g):
        slot = g % 2
        p, a = part, ag.at[g % AG_SLOTS]
        lb, rb, fb = block(left_chip), block(right_chip), block(far_chip)
        mine, from_left, from_right = sub(chip), sub(left_chip), sub(right_chip)
        table = {
            SIB: (p.at[sib_half], rsib, sib),
            M1L: (p.at[fb, first], ro.at[slot, 0], left),
            M1R: (p.at[fb, second], ro.at[slot, 1], right),
            M2L: (p.at[lb, second], rf.at[slot, 0, :, second], left),
            M2R: (p.at[rb, first], rf.at[slot, 1, :, first], right),
            M3L: (m3.at[0], rf.at[slot, 0, :, first], left),
            M3R: (m3.at[1], rf.at[slot, 1, :, second], right),
            A1L: (a.at[mine, first], a.at[mine, first], left),
            A1R: (a.at[mine, second], a.at[mine, second], right),
            A2L: (a.at[mine, second], a.at[mine, second], left),
            A2R: (a.at[mine, first], a.at[mine, first], right),
            A3L: (a.at[from_right, first], a.at[from_right, first], left),
            A3R: (a.at[from_left, second], a.at[from_left, second], right),
        }
        return lambda kind: msg(kind, g % AG_SLOTS if kind >= A1L else slot, *table[kind])

    def chunk_rows(g):
        return pl.ds(pl.multiple_of((g % n_chunks) * rows, rows), rows)

    def weight_copies(which, layer):
        groups = {
            "qkv": [
                (wq_ref.at[layer], wqkv.at[:, pl.ds(0, qw)], 0),
                (wk_ref.at[layer], wqkv.at[:, pl.ds(qw, HEAD_DIM)], 1),
                (wv_ref.at[layer], wqkv.at[:, pl.ds(qw + HEAD_DIM, HEAD_DIM)], 2),
            ],
            "ff": [(wg_ref.at[layer], wg, 3), (wu_ref.at[layer], wu, 4)],
            "od": [(wo_ref.at[layer], wod.at[pl.ds(0, qw)], 5), (wd_ref.at[layer], wod.at[pl.ds(qw, ff)], 6)],
        }
        return [pltpu.make_async_copy(src, dst, w_sem.at[n]) for src, dst, n in groups[which]]

    def start_input(g):
        r = chunk_rows(g)

        @pl.when(g < n_chunks)
        def _():
            pltpu.make_async_copy(x_ref.at[r], xn, in_sem.at[0]).start()

        @pl.when(g >= n_chunks)
        def _():
            pltpu.make_async_copy(h_ref.at[g // n_chunks - 1, r], xn, in_sem.at[0]).start()

        pltpu.make_async_copy(pos_ref.at[r], pos, in_sem.at[1]).start()

    def wait_input(g):
        r = chunk_rows(g)
        pltpu.make_async_copy(x_ref.at[r], xn, in_sem.at[0]).wait()
        pltpu.make_async_copy(pos_ref.at[r], pos, in_sem.at[1]).wait()

    def seq_start(g):
        return pl.multiple_of((g % per_seq) * rows, rows)

    def kv_copies(g):
        here = pl.ds(seq_start(g), rows)
        r = chunk_rows(g)
        return [
            pltpu.make_async_copy(k_scr.at[here, pl.ds(0, HEAD_DIM)], kc_ref.at[g // n_chunks, r], kv_sem.at[0]),
            pltpu.make_async_copy(v_scr.at[here, pl.ds(0, HEAD_DIM)], vc_ref.at[g // n_chunks, r], kv_sem.at[1]),
        ]

    def gathered(g):
        src = ag.at[g % AG_SLOTS]
        dst = pl.ds(pl.multiple_of((g % n_chunks) * rows + my_base, hrows), hrows)
        slot = g % AG_SLOTS
        last = g >= total - n_chunks

        def copies(ref):
            return pltpu.make_async_copy(src, ref.at[dst], ago_sem.at[slot]), msg(AS, slot, src, ref.at[dst], sib)

        def start():
            @pl.when(last)
            def _():
                for copy in copies(y_ref):
                    copy.start()

            @pl.when(jnp.logical_not(last))
            def _():
                for copy in copies(h_ref.at[g // n_chunks]):
                    copy.start()

        return start, copies

    def residual_copy(c):
        src = pl.ds(pl.multiple_of(c * rows + my_base + chip * quarter, quarter), quarter)
        return pltpu.make_async_copy(x_ref.at[src], hres.at[c], res_sem.at[c])

    def reduce_first(g):
        slot = g % 2
        m = messages(g)
        m(SIB).wait_recv()
        p, s = part, rsib

        def fold(chip_id):
            b = block(chip_id)
            p[b, :] = (p[b, :].astype(F32) + s[sub(chip_id), :].astype(F32)).astype(BF16)

        fold(far_chip)
        m(M1L).start()
        m(M1R).start()
        fold(left_chip)
        m(M2L).start()
        fold(right_chip)
        m(M2R).start()
        own[slot] = p[block(chip), :].astype(F32) + s[sub(chip), :].astype(F32)

        @pl.when(g < total - 1)
        def _():
            pl.semaphore_signal(credit, inc=1, device_id={"tp": sib}, device_id_type=MESH)

    def reduce_second(g):
        slot = g % 2
        m = messages(g)
        m(M1L).wait_recv()
        m3[0] = (part[block(left_chip), first].astype(F32) + ro[slot, 0].astype(F32)).astype(BF16)
        m(M3L).start()
        m(M1R).wait_recv()
        m3[1] = (part[block(right_chip), second].astype(F32) + ro[slot, 1].astype(F32)).astype(BF16)
        m(M3R).start()

    def reduce_last(g):
        slot = g % 2
        c = g % n_chunks
        m = messages(g)
        for kind in (M2L, M2R, M3L, M3R):
            m(kind).wait_recv()

        @pl.when(g < n_chunks)
        def _():
            residual_copy(c).wait()

        h = (own[slot] + (rf[slot, 0].astype(F32) + rf[slot, 1].astype(F32)) + hres[c].astype(F32)).astype(BF16)
        hres[c] = h
        ag[g % AG_SLOTS, sub(chip), :] = h
        for kind in (A1L, A1R, A2L, A2R):
            m(kind).start()

    def gather_forward(g):
        m = messages(g)
        m(A1L).wait_recv()
        m(A3L).start()
        m(A1R).wait_recv()
        m(A3R).start()

    def gather_last(g):
        slot = g % 2
        m = messages(g)
        for kind in (A2L, A2R, A3L, A3R):
            m(kind).wait_recv()
        gathered(g)[0]()

    def gather_sibling(g):
        gathered(g)[1](y_ref)[1].wait_recv()

    def gather_done(g):
        m = messages(g)
        for kind in (A1L, A1R, A2L, A2R, A3L, A3R):
            m(kind).wait_send()
        local, remote = gathered(g)[1](y_ref)
        local.wait()
        remote.wait_send()

    def first_done(g):
        m = messages(g)
        for kind in (SIB, M1L, M1R, M2L, M2R):
            m(kind).wait_send()

    def second_done(g):
        m = messages(g)
        for kind in (M3L, M3R):
            m(kind).wait_send()

    def guarded(g, fn):
        @pl.when(jnp.logical_and(g >= 0, g < total))
        def _():
            fn(g)

    def normalize(g, part_idx, n_parts):
        size = rows // n_parts
        rr = pl.ds(part_idx * size, size)
        gain = ng_ref[pl.ds(jnp.minimum(g // n_chunks, n_layers - 1), 1), :]
        xn[rr, :] = norm_last(xn[rr, :].astype(F32), gain).astype(BF16)

    def expand(g):
        n = xn[...]
        layer = g // n_chunks
        here = pl.ds(seq_start(g), rows)
        cos, sin = cos_sin(pos[...] * fr_ref[0:1, :])
        cs[...] = cos
        sn[...] = sin * fr_ref[1:2, :]

        def head(values, gain):
            return rope(norm_last(values, gain), cs[...], sn[...]).astype(BF16)

        def put_k(values):
            k_scr[here, :HEAD_DIM] = head(values, kg_ref[layer])

        def put_q(hd):
            def put(values):
                q_scr[hd, :, :HEAD_DIM] = head(values, qg_ref[layer, hd:hd + 1, :])
            return put

        z = mm(n, wqkv[:, qw:qw + 2 * HEAD_DIM])
        v_scr[here, :HEAD_DIM] = z[:, HEAD_DIM:].astype(BF16)
        pending = [(put_k, z[:, :HEAD_DIM])]
        row_id = seq_start(g) + lax.broadcasted_iota(jnp.int32, (rows, HEAD_DIM), 0)
        lane = lax.broadcasted_iota(jnp.int32, (rows, HEAD_DIM), 1)
        length = len_ref[(g % n_chunks) // per_seq]
        k_scr[here, HEAD_DIM:] = jnp.where(jnp.logical_and(lane == 0, row_id >= length), NEG, 0.0).astype(BF16)
        for pair in range(heads // 2):
            z = mm(n, wqkv[:, pair * 2 * HEAD_DIM:(pair + 1) * 2 * HEAD_DIM])
            pending += [(put_q(2 * pair + e), z[:, e * HEAD_DIM:(e + 1) * HEAD_DIM]) for e in range(2)]
        for c0 in range(0, ff, 256):
            c1 = min(c0 + 256, ff)
            gate = mm_t(n, wg[c0:c1, :])
            up = mm_t(n, wu[c0:c1, :])
            if pending:
                put, values = pending.pop(0)
                put(values)
            act[:, qw + c0:qw + c1] = (jax.nn.silu(gate) * up).astype(BF16)
        for put, values in pending:
            put(values)

    def attention(g):
        s0 = seq_start(g)
        lanes = HEAD_DIM

        def stream(units, scores, soft, weigh):
            following, last = scores(units[0]), None
            for n, unit in enumerate(units):
                current = following
                if n + 1 < len(units):
                    following = scores(units[n + 1])
                probs = soft(unit, current)
                if last is not None:
                    weigh(*last)
                last = (unit, probs)
            weigh(*last)

        def top_of(tiles):
            top = tiles[0]
            for t in tiles[1:]:
                top = jnp.maximum(top, t)
            return jnp.max(top, axis=-1, keepdims=True)

        def probs_of(tiles, top):
            return jnp.concatenate([jnp.exp2((t - top) * c_exp).astype(BF16) for t in tiles], axis=1)

        size = rows // 2
        offset = lax.broadcasted_iota(jnp.int32, (size, lanes), 0) - lax.broadcasted_iota(jnp.int32, (size, lanes), 1)

        def own_keys(part_idx):
            return pl.ds(s0, (part_idx + 1) * size)

        def own_scores(unit):
            hd, n = unit
            return mm_t(q_scr[hd, n * size:(n + 1) * size, :], k_scr[own_keys(n), :])

        def own_soft(unit, s):
            hd, n = unit
            tiles = []
            for t in range(0, (n + 1) * size, lanes):
                tile = s[:, t:t + lanes]
                tiles.append(tile if t + lanes <= n * size else jnp.where(offset >= t - n * size, tile, NEG))
            top = top_of(tiles)
            m_scr[hd, n * size:(n + 1) * size, :] = jnp.broadcast_to(top, (size, lanes))
            return probs_of(tiles, top)

        def own_weigh(unit, p):
            hd, n = unit
            acc_scr[hd, n * size:(n + 1) * size, :] = mm(p, v_scr[own_keys(n), :])

        stream([(hd, n) for hd in range(heads) for n in range(2)], own_scores, own_soft, own_weigh)

        def body(j, carry):
            keys = pl.ds(pl.multiple_of(j * rows, rows), rows)

            def scores(hd):
                return mm_t(q_scr[hd], k_scr[keys, :])

            def soft(hd, s):
                tiles = [s[:, t:t + lanes] for t in range(0, rows, lanes)]
                old = m_scr[hd]
                top = jnp.maximum(old, top_of(tiles))
                m_scr[hd] = top
                return probs_of(tiles, top), jnp.exp2((old - top) * c_exp)

            def weigh(hd, probs):
                p, scale = probs
                pv = mm(p, v_scr[keys, :])
                acc_scr[hd, :, :lanes] = acc_scr[hd, :, :lanes] * scale + pv[:, :lanes]
                acc_scr[hd, :, lanes:] = acc_scr[hd, :, lanes:] * scale + pv[:, lanes:]

            stream(list(range(heads)), scores, soft, weigh)
            return carry

        lax.fori_loop(0, g % per_seq, body, 0)
        for hd in range(heads):
            out = acc_scr[hd, :, :lanes] / acc_scr[hd, :, lanes:]
            act[:, hd * lanes:(hd + 1) * lanes] = out.astype(BF16)

    def output(g, side):
        p = part
        r = (sib_half, my_half)[side]
        a = act[r, :]
        n_cols = 2
        step = width // n_cols
        for n in range(n_cols):
            p[r, n * step:(n + 1) * step] = mm(a, wod[:, n * step:(n + 1) * step]).astype(BF16)
            normalize(g + 1, 2 * side + n, 4)

    def layer_start(g, which):
        @pl.when(g % n_chunks == 0)
        def _():
            for copy in weight_copies(which, g // n_chunks):
                copy.wait()

    def layer_end(g, which):
        @pl.when(jnp.logical_and(g % n_chunks == n_chunks - 1, g < total - 1))
        def _():
            for copy in weight_copies(which, g // n_chunks + 1):
                copy.start()

    start_input(0)
    for copy in weight_copies("qkv", 0):
        copy.start()
    barrier = pltpu.get_barrier_semaphore()
    for dev in (left, right, sib):
        pl.semaphore_signal(barrier, inc=1, device_id={"tp": dev}, device_id_type=MESH)
    q_scr[:, :, HEAD_DIM:] = jnp.ones((heads, rows, HEAD_DIM), BF16)
    v_scr[:, HEAD_DIM:] = jnp.ones((v_scr.shape[0], HEAD_DIM), BF16)
    pad = act.shape[1] - (qw + ff)
    if pad:
        act[:, qw + ff:] = jnp.zeros((rows, pad), BF16)
        wod[qw + ff:, :] = jnp.zeros((pad, width), BF16)
    wait_input(0)
    for which in ("ff", "od"):
        for copy in weight_copies(which, 0):
            copy.start()
    for n in range(4):
        normalize(0, n, 4)
    for c in range(n_chunks):
        residual_copy(c).start()
    pl.semaphore_wait(barrier, 3)

    def step(i, carry):
        busy = i < total

        @pl.when(busy)
        def _():
            layer_start(i, "qkv")
            layer_start(i, "ff")
            expand(i)
            layer_end(i, "qkv")
            layer_end(i, "ff")
            for copy in kv_copies(i):
                copy.start()

            @pl.when(i + 1 < total)
            def _():
                start_input(i + 1)

            attention(i)
            for copy in kv_copies(i):
                copy.wait()

        guarded(i - 4, gather_done)
        guarded(i - 2, second_done)
        guarded(i - 1, reduce_second)
        guarded(i - 2, gather_forward)
        guarded(i - 3, gather_last)
        guarded(i - 1, first_done)

        @pl.when(busy)
        def _():
            layer_start(i, "od")

            @pl.when(i + 1 < total)
            def _():
                wait_input(i + 1)

            output(i, 0)

            @pl.when(i > 0)
            def _():
                pl.semaphore_wait(credit, 1)

            messages(i)(SIB).start()
            output(i, 1)
            layer_end(i, "od")

        guarded(i, reduce_first)
        guarded(i - 1, reduce_last)
        guarded(i - 3, gather_sibling)
        return carry

    lax.fori_loop(0, total + 4, step, 0)


def run_layers(x, positions, lengths, w_q, w_k, w_v, w_o, w_gate, w_up, w_down, norm_gain, q_gain, k_gain, n_tp):
    n_batch, seq, width = x.shape
    n_layers = w_q.shape[0]
    heads = w_q.shape[2] // HEAD_DIM
    ff = w_gate.shape[2]
    rows = min(CHUNK_ROWS, seq // 4)
    tokens = n_batch * seq
    n_chunks, per_seq, chips = tokens // rows, seq // rows, n_tp // 2
    quarter = rows // n_tp
    act_width = -(-(heads * HEAD_DIM + ff) // 256) * 256
    cfg = (n_layers, n_chunks, rows, per_seq, heads, chips)
    lane = jnp.arange(HEAD_DIM)
    freqs = jnp.stack([ROPE_THETA ** (-((lane // 2).astype(F32) * (2.0 / HEAD_DIM))), jnp.where(lane % 2 == 0, -1.0, 1.0).astype(F32)])
    pos = jnp.broadcast_to(positions.reshape(tokens, 1).astype(F32), (tokens, HEAD_DIM))
    any_spec = pl.BlockSpec(memory_space=pl.ANY)
    vmem_spec = pl.BlockSpec(memory_space=pltpu.VMEM)
    dma = pltpu.SemaphoreType.DMA
    h, y, kc, vc = pl.pallas_call(
        functools.partial(layers_kernel, cfg),
        name="layers",
        out_shape=(
            jax.ShapeDtypeStruct((max(n_layers - 1, 1), tokens, width), BF16),
            jax.ShapeDtypeStruct((tokens, width), BF16),
            jax.ShapeDtypeStruct((n_layers, tokens, HEAD_DIM), BF16),
            jax.ShapeDtypeStruct((n_layers, tokens, HEAD_DIM), BF16),
        ),
        in_specs=[pl.BlockSpec(memory_space=pltpu.SMEM)] + [any_spec] * 9 + [vmem_spec] * 4,
        out_specs=(any_spec,) * 4,
        scratch_shapes=[
            pltpu.VMEM((width, (heads + 2) * HEAD_DIM), BF16),
            pltpu.VMEM((ff, width), BF16),
            pltpu.VMEM((ff, width), BF16),
            pltpu.VMEM((act_width, width), BF16),
            pltpu.VMEM((rows, width), BF16),
            pltpu.VMEM((rows, HEAD_DIM), F32),
            pltpu.VMEM((rows, HEAD_DIM), F32),
            pltpu.VMEM((rows, HEAD_DIM), F32),
            pltpu.VMEM((rows, act_width), BF16),
            pltpu.VMEM((heads, rows, 2 * HEAD_DIM), BF16),
            pltpu.VMEM((seq, 2 * HEAD_DIM), BF16),
            pltpu.VMEM((seq, 2 * HEAD_DIM), BF16),
            pltpu.VMEM((heads, rows, HEAD_DIM), F32),
            pltpu.VMEM((heads, rows, 2 * HEAD_DIM), F32),
            pltpu.VMEM((rows, width), BF16),
            pltpu.VMEM((rows // 2, width), BF16),
            pltpu.VMEM((2, quarter, width // 2), BF16),
            pltpu.VMEM((2, quarter, width), F32),
            pltpu.VMEM((2, 2, quarter, width // 2), BF16),
            pltpu.VMEM((2, 2, quarter, width), BF16),
            pltpu.VMEM((AG_SLOTS, rows // 2, width), BF16),
            pltpu.VMEM((n_chunks, quarter, width), BF16),
            dma((7,)), dma((2,)), dma((2,)), dma((n_chunks,)), dma((AG_SLOTS,)), dma((N_MSG, AG_SLOTS)), dma((N_MSG, AG_SLOTS)),
            pltpu.SemaphoreType.REGULAR,
        ],
        compiler_params=pltpu.CompilerParams(collective_id=0, has_side_effects=True, vmem_limit_bytes=67043328),
    )(
        lengths, x.reshape(tokens, width), pos, w_q, w_k, w_v, w_o, jnp.swapaxes(w_gate, 1, 2), jnp.swapaxes(w_up, 1, 2), w_down,
        norm_gain, q_gain, k_gain, freqs
    )
    y = y.reshape(n_batch, seq, width)
    cache_shape = (n_layers, n_batch, seq, 1, HEAD_DIM)
    return y, kc.reshape(cache_shape), vc.reshape(cache_shape)


def solution(mesh):
    act_spec = P('dp', None, None)
    col_spec = P(None, None, 'tp')
    row_spec = P(None, 'tp', None)
    cache_spec = P(None, 'dp', None, 'tp', None)
    in_specs = (act_spec, P('dp', None), P('dp'), col_spec, col_spec, col_spec, row_spec, col_spec, col_spec, row_spec, P(None, None), row_spec, row_spec)
    n_tp = mesh.shape['tp']

    def device_body(x, positions, lengths, w_q, w_k, w_v, w_o, w_gate, w_up, w_down, norm_gain, q_gain, k_gain):
        return run_layers(x, positions, lengths, w_q, w_k, w_v, w_o, w_gate, w_up, w_down, norm_gain, q_gain, k_gain, n_tp)

    return jax.shard_map(device_body, mesh=mesh, in_specs=in_specs, out_specs=(act_spec, cache_spec, cache_spec), check_vma=False)
```

```python
import functools

import jax
import jax.numpy as jnp
import numpy as np
from jax import lax
from jax.experimental import pallas as pl
from jax.experimental.pallas import tpu as pltpu
from jax.sharding import PartitionSpec as P

HEAD_DIM = 128
ROPE_THETA = 75000000.0
NORM_EPS = 1e-5
NEG = -1e30
LOG2E = 1.4426950408889634
CHUNK_ROWS = 512
AG_SLOTS = 3
MESH = pl.DeviceIdType.MESH
F32 = jnp.float32
BF16 = jnp.bfloat16

SIB, M1L, M1R, M2L, M2R, M3L, M3R, A1L, A1R, A2L, A2R, A3L, A3R, AS = range(14)
N_MSG = 14


def mm(a, b):
    return jnp.dot(a, b, preferred_element_type=F32)


def mm_t(a, b):
    return lax.dot_general(a, b, (((1,), (1,)), ((), ())), preferred_element_type=F32)


def norm_last(values, gain):
    width = values.shape[-1]
    mean = jnp.sum(values, axis=-1, keepdims=True) * (1.0 / width)
    centered = values - mean
    var = jnp.sum(centered * centered, axis=-1, keepdims=True) * (1.0 / width)
    return centered * lax.rsqrt(var + NORM_EPS) * gain


def cos_sin(angles):
    turns = jnp.round(angles * 0.6366197723675814)
    r = ((angles - turns * 1.5703125) - turns * 4.837512969970703e-4) - turns * 7.549789954891882e-8
    r2 = r * r
    sin_r = r + r * r2 * (-1.6666654611e-1 + r2 * (8.3321608736e-3 - r2 * 1.9515295891e-4))
    cos_r = 1.0 - 0.5 * r2 + r2 * r2 * (4.166664568298827e-2 + r2 * (-1.388731625493765e-3 + r2 * 2.443315711809948e-5))
    quad = turns.astype(jnp.int32) & 3
    odd = (quad & 1) == 1
    cos = jnp.where(odd, sin_r, cos_r)
    sin = jnp.where(odd, cos_r, sin_r)
    cos = jnp.where((quad == 1) | (quad == 2), -cos, cos)
    sin = jnp.where(quad >= 2, -sin, sin)
    return cos, sin


def rope(values, cos, sin):
    lane = lax.broadcasted_iota(jnp.int32, values.shape, 1)
    swapped = jnp.where(lane % 2 == 0, pltpu.roll(values, HEAD_DIM - 1, 1), pltpu.roll(values, 1, 1))
    return values * cos + swapped * sin


def layers_kernel(
    cfg,
    len_ref, x_ref, wq_ref, wk_ref, wv_ref, wo_ref, wg_ref, wu_ref, wd_ref, pos_ref, ng_ref, qg_ref, kg_ref, fr_ref,
    h_ref, y_ref, kc_ref, vc_ref,
    wqkv, wg, wu, wod, xn, cs, sn, act, q_scr, k_scr, v_scr, m_scr, acc_scr, part, rsib, m3, own, ro, rf, ag, hres,
    w_sem, in_sem, kv_sem, res_sem, ago_sem, s_sem, r_sem, credit,
):
    n_layers, n_chunks, rows, per_seq, heads, chips = cfg
    width = x_ref.shape[1]
    half = width // 2
    ff = wg_ref.shape[1]
    qw = heads * HEAD_DIM
    quarter = rows // (2 * chips)
    hrows = rows // 2
    total = n_layers * n_chunks
    c_exp = HEAD_DIM ** -0.5 * LOG2E

    me = lax.axis_index("tp")
    chip, core = me // 2, me % 2
    left_chip, right_chip, far_chip = (chip + chips - 1) % chips, (chip + 1) % chips, (chip + 2) % chips
    left, right, sib = left_chip * 2 + core, right_chip * 2 + core, chip * 2 + 1 - core
    my_base, sib_base = core * hrows, (1 - core) * hrows

    def block(chip_id):
        return pl.ds(pl.multiple_of(my_base + chip_id * quarter, quarter), quarter)

    def sub(chip_id):
        return pl.ds(pl.multiple_of(chip_id * quarter, quarter), quarter)

    my_half = pl.ds(pl.multiple_of(my_base, hrows), hrows)
    sib_half = pl.ds(pl.multiple_of(sib_base, hrows), hrows)
    first, second = pl.ds(0, half), pl.ds(half, half)

    def msg(kind, slot, src, dst, dev):
        return pltpu.make_async_remote_copy(
            src_ref=src, dst_ref=dst, send_sem=s_sem.at[kind, slot], recv_sem=r_sem.at[kind, slot],
            device_id={"tp": dev}, device_id_type=MESH,
        )

    def messages(g):
        slot = g % 2
        p, a = part, ag.at[g % AG_SLOTS]
        lb, rb, fb = block(left_chip), block(right_chip), block(far_chip)
        mine, from_left, from_right = sub(chip), sub(left_chip), sub(right_chip)
        table = {
            SIB: (p.at[sib_half], rsib, sib),
            M1L: (p.at[fb, first], ro.at[slot, 0], left),
            M1R: (p.at[fb, second], ro.at[slot, 1], right),
            M2L: (p.at[lb, second], rf.at[slot, 0, :, second], left),
            M2R: (p.at[rb, first], rf.at[slot, 1, :, first], right),
            M3L: (m3.at[0], rf.at[slot, 0, :, first], left),
            M3R: (m3.at[1], rf.at[slot, 1, :, second], right),
            A1L: (a.at[mine, first], a.at[mine, first], left),
            A1R: (a.at[mine, second], a.at[mine, second], right),
            A2L: (a.at[mine, second], a.at[mine, second], left),
            A2R: (a.at[mine, first], a.at[mine, first], right),
            A3L: (a.at[from_right, first], a.at[from_right, first], left),
            A3R: (a.at[from_left, second], a.at[from_left, second], right),
        }
        return lambda kind: msg(kind, g % AG_SLOTS if kind >= A1L else slot, *table[kind])

    def chunk_rows(g):
        return pl.ds(pl.multiple_of((g % n_chunks) * rows, rows), rows)

    def weight_copies(which, layer):
        groups = {
            "qkv": [
                (wq_ref.at[layer], wqkv.at[:, pl.ds(0, qw)], 0),
                (wk_ref.at[layer], wqkv.at[:, pl.ds(qw, HEAD_DIM)], 1),
                (wv_ref.at[layer], wqkv.at[:, pl.ds(qw + HEAD_DIM, HEAD_DIM)], 2),
            ],
            "ff": [(wg_ref.at[layer], wg, 3), (wu_ref.at[layer], wu, 4)],
            "od": [(wo_ref.at[layer], wod.at[pl.ds(0, qw)], 5), (wd_ref.at[layer], wod.at[pl.ds(qw, ff)], 6)],
        }
        return [pltpu.make_async_copy(src, dst, w_sem.at[n]) for src, dst, n in groups[which]]

    def start_input(g):
        r = chunk_rows(g)

        @pl.when(g < n_chunks)
        def _():
            pltpu.make_async_copy(x_ref.at[r], xn, in_sem.at[0]).start()

        @pl.when(g >= n_chunks)
        def _():
            pltpu.make_async_copy(h_ref.at[g // n_chunks - 1, r], xn, in_sem.at[0]).start()

    def wait_input(g):
        pltpu.make_async_copy(x_ref.at[chunk_rows(g)], xn, in_sem.at[0]).wait()

    def seq_start(g):
        return pl.multiple_of((g % per_seq) * rows, rows)

    def kv_copies(g):
        here = pl.ds(seq_start(g), rows)
        r = chunk_rows(g)
        return [
            pltpu.make_async_copy(k_scr.at[here, pl.ds(0, HEAD_DIM)], kc_ref.at[g // n_chunks, r], kv_sem.at[0]),
            pltpu.make_async_copy(v_scr.at[here, pl.ds(0, HEAD_DIM)], vc_ref.at[g // n_chunks, r], kv_sem.at[1]),
        ]

    def gathered(g):
        src = ag.at[g % AG_SLOTS]
        dst = pl.ds(pl.multiple_of((g % n_chunks) * rows + my_base, hrows), hrows)
        slot = g % AG_SLOTS
        last = g >= total - n_chunks

        def copies(ref):
            return pltpu.make_async_copy(src, ref.at[dst], ago_sem.at[slot]), msg(AS, slot, src, ref.at[dst], sib)

        def start():
            @pl.when(last)
            def _():
                for copy in copies(y_ref):
                    copy.start()

            @pl.when(jnp.logical_not(last))
            def _():
                for copy in copies(h_ref.at[g // n_chunks]):
                    copy.start()

        return start, copies

    def residual_copy(c):
        src = pl.ds(pl.multiple_of(c * rows + my_base + chip * quarter, quarter), quarter)
        return pltpu.make_async_copy(x_ref.at[src], hres.at[c], res_sem.at[c])

    def reduce_first(g):
        slot = g % 2
        m = messages(g)
        m(SIB).wait_recv()
        p, s = part, rsib

        def fold(chip_id):
            b = block(chip_id)
            p[b, :] = (p[b, :].astype(F32) + s[sub(chip_id), :].astype(F32)).astype(BF16)

        fold(far_chip)
        m(M1L).start()
        m(M1R).start()
        fold(left_chip)
        m(M2L).start()
        fold(right_chip)
        m(M2R).start()
        own[slot] = p[block(chip), :].astype(F32) + s[sub(chip), :].astype(F32)

        @pl.when(g < total - 1)
        def _():
            pl.semaphore_signal(credit, inc=1, device_id={"tp": sib}, device_id_type=MESH)

    def reduce_second(g):
        slot = g % 2
        m = messages(g)
        m(M1L).wait_recv()
        m3[0] = (part[block(left_chip), first].astype(F32) + ro[slot, 0].astype(F32)).astype(BF16)
        m(M3L).start()
        m(M1R).wait_recv()
        m3[1] = (part[block(right_chip), second].astype(F32) + ro[slot, 1].astype(F32)).astype(BF16)
        m(M3R).start()

    def reduce_last(g):
        slot = g % 2
        c = g % n_chunks
        m = messages(g)
        for kind in (M2L, M2R, M3L, M3R):
            m(kind).wait_recv()

        @pl.when(g < n_chunks)
        def _():
            residual_copy(c).wait()

        h = (own[slot] + (rf[slot, 0].astype(F32) + rf[slot, 1].astype(F32)) + hres[c].astype(F32)).astype(BF16)
        hres[c] = h
        ag[g % AG_SLOTS, sub(chip), :] = h
        for kind in (A1L, A1R):
            m(kind).start()

    def gather_second(g):
        m = messages(g)
        for kind in (A2L, A2R):
            m(kind).start()

    def gather_forward(g):
        m = messages(g)
        m(A1L).wait_recv()
        m(A3L).start()
        m(A1R).wait_recv()
        m(A3R).start()

    def gather_last(g):
        slot = g % 2
        m = messages(g)
        for kind in (A2L, A2R, A3L, A3R):
            m(kind).wait_recv()
        gathered(g)[0]()

    def gather_sibling(g):
        gathered(g)[1](y_ref)[1].wait_recv()

    def gather_done(g):
        m = messages(g)
        for kind in (A1L, A1R, A2L, A2R, A3L, A3R):
            m(kind).wait_send()
        local, remote = gathered(g)[1](y_ref)
        local.wait()
        remote.wait_send()

    def first_done(g):
        m = messages(g)
        for kind in (SIB, M1L, M1R, M2L, M2R):
            m(kind).wait_send()

    def second_done(g):
        m = messages(g)
        for kind in (M3L, M3R):
            m(kind).wait_send()

    def guarded(g, fn):
        @pl.when(jnp.logical_and(g >= 0, g < total))
        def _():
            fn(g)

    def normalize(g, part_idx, n_parts):
        size = rows // n_parts
        rr = pl.ds(part_idx * size, size)
        gain = ng_ref[pl.ds(jnp.minimum(g // n_chunks, n_layers - 1), 1), :]
        xn[rr, :] = norm_last(xn[rr, :].astype(F32), gain).astype(BF16)

    def expand(g):
        n = xn[...]
        layer = g // n_chunks
        here = pl.ds(seq_start(g), rows)
        for n_row in range(rows // HEAD_DIM):
            row = pos_ref[pl.ds((g % n_chunks) * (rows // HEAD_DIM) + n_row, 1), :].astype(F32)
            down = jnp.transpose(jnp.broadcast_to(row, (HEAD_DIM, HEAD_DIM)))
            cos, sin = cos_sin(down * fr_ref[0:1, :])
            part_rows = slice(n_row * HEAD_DIM, (n_row + 1) * HEAD_DIM)
            cs[part_rows, :] = cos
            sn[part_rows, :] = sin * fr_ref[1:2, :]

        def head(values, gain):
            return rope(norm_last(values, gain), cs[...], sn[...]).astype(BF16)

        def put_k(values):
            k_scr[here, :HEAD_DIM] = head(values, kg_ref[layer])

        def put_q(hd):
            def put(values):
                q_scr[hd, :, :HEAD_DIM] = head(values, qg_ref[layer, hd:hd + 1, :])
            return put

        z = mm(n, wqkv[:, qw:qw + 2 * HEAD_DIM])
        v_scr[here, :HEAD_DIM] = z[:, HEAD_DIM:].astype(BF16)
        pending = [(put_k, z[:, :HEAD_DIM])]
        row_id = seq_start(g) + lax.broadcasted_iota(jnp.int32, (rows, HEAD_DIM), 0)
        lane = lax.broadcasted_iota(jnp.int32, (rows, HEAD_DIM), 1)
        length = len_ref[(g % n_chunks) // per_seq]
        k_scr[here, HEAD_DIM:] = jnp.where(jnp.logical_and(lane == 0, row_id >= length), NEG, 0.0).astype(BF16)
        for pair in range(heads // 2):
            z = mm(n, wqkv[:, pair * 2 * HEAD_DIM:(pair + 1) * 2 * HEAD_DIM])
            pending += [(put_q(2 * pair + e), z[:, e * HEAD_DIM:(e + 1) * HEAD_DIM]) for e in range(2)]
        for c0 in range(0, ff, 256):
            c1 = min(c0 + 256, ff)
            gate = mm_t(n, wg[c0:c1, :])
            up = mm_t(n, wu[c0:c1, :])
            if pending:
                put, values = pending.pop(0)
                put(values)
            act[:, qw + c0:qw + c1] = (jax.nn.silu(gate) * up).astype(BF16)
        for put, values in pending:
            put(values)

    def attention(g):
        s0 = seq_start(g)
        lanes = HEAD_DIM
        size = min(rows, 256)

        def stream(units, scores, soft, weigh):
            following, last = scores(units[0]), None
            for n, unit in enumerate(units):
                current = following
                if n + 1 < len(units):
                    following = scores(units[n + 1])
                probs = soft(unit, current)
                if last is not None:
                    weigh(*last)
                last = (unit, probs)
            weigh(*last)

        def top_of(tiles):
            top = tiles[0]
            for t in tiles[1:]:
                top = jnp.maximum(top, t)
            return jnp.max(top, axis=-1, keepdims=True)

        def probs_of(tiles, top):
            return jnp.concatenate([jnp.exp2((t - top) * c_exp).astype(BF16) for t in tiles], axis=1)

        step = 2 * size
        n_units = rows // size
        offset = lax.broadcasted_iota(jnp.int32, (size, lanes), 0) - lax.broadcasted_iota(jnp.int32, (size, lanes), 1)

        def own(first_half):
            base = pl.multiple_of(s0 - first_half * size, size)

            def own_keys(n):
                return pl.ds(base, (first_half + n + 1) * size)

            def own_scores(unit):
                hd, n = unit
                return mm_t(q_scr[hd, n * size:(n + 1) * size, :], k_scr[own_keys(n), :])

            def own_soft(unit, s):
                hd, n = unit
                before = (first_half + n) * size
                tiles = []
                for t in range(0, before + size, lanes):
                    tile = s[:, t:t + lanes]
                    tiles.append(tile if t < before else jnp.where(offset >= t - before, tile, NEG))
                top = top_of(tiles)
                m_scr[hd, n * size:(n + 1) * size, :] = jnp.broadcast_to(top, (size, lanes))
                return probs_of(tiles, top)

            def own_weigh(unit, p):
                hd, n = unit
                acc_scr[hd, n * size:(n + 1) * size, :] = mm(p, v_scr[own_keys(n), :])

            stream([(hd, n) for hd in range(heads) for n in range(n_units)], own_scores, own_soft, own_weigh)

        if n_units == 2:
            own(0)
        else:
            for odd in range(2):
                @pl.when((s0 // size) % 2 == odd)
                def _():
                    own(odd)

        def body(j, carry):
            keys = pl.ds(pl.multiple_of(j * step, step), step)

            def scores(hd):
                return mm_t(q_scr[hd], k_scr[keys, :])

            def soft(hd, s):
                tiles = [s[:, t:t + lanes] for t in range(0, step, lanes)]
                old = m_scr[hd]
                top = jnp.maximum(old, top_of(tiles))
                m_scr[hd] = top
                return probs_of(tiles, top), jnp.exp2((old - top) * c_exp)

            def weigh(hd, probs):
                p, scale = probs
                pv = mm(p, v_scr[keys, :])
                acc_scr[hd, :, :lanes] = acc_scr[hd, :, :lanes] * scale + pv[:, :lanes]
                acc_scr[hd, :, lanes:] = acc_scr[hd, :, lanes:] * scale + pv[:, lanes:]

            stream(list(range(heads)), scores, soft, weigh)
            return carry

        lax.fori_loop(0, s0 // step, body, 0)
        for hd in range(heads):
            out = acc_scr[hd, :, :lanes] / acc_scr[hd, :, lanes:]
            act[:, hd * lanes:(hd + 1) * lanes] = out.astype(BF16)

    def output(g, side):
        p = part
        r = (sib_half, my_half)[side]
        a = act[r, :]
        n_cols = 2
        step = width // n_cols
        for n in range(n_cols):
            p[r, n * step:(n + 1) * step] = mm(a, wod[:, n * step:(n + 1) * step]).astype(BF16)
            normalize(g + 1, 2 * side + n, 4)

    def layer_start(g, which):
        @pl.when(g % n_chunks == 0)
        def _():
            for copy in weight_copies(which, g // n_chunks):
                copy.wait()

    def layer_end(g, which):
        @pl.when(jnp.logical_and(g % n_chunks == n_chunks - 1, g < total - 1))
        def _():
            for copy in weight_copies(which, g // n_chunks + 1):
                copy.start()

    start_input(0)
    for copy in weight_copies("qkv", 0) + weight_copies("ff", 0):
        copy.start()
    barrier = pltpu.get_barrier_semaphore()
    for dev in (left, right, sib):
        pl.semaphore_signal(barrier, inc=1, device_id={"tp": dev}, device_id_type=MESH)
    q_scr[:, :, HEAD_DIM:] = jnp.ones((heads, rows, HEAD_DIM), BF16)
    v_scr[:, HEAD_DIM:] = jnp.ones((v_scr.shape[0], HEAD_DIM), BF16)
    pad = act.shape[1] - (qw + ff)
    if pad:
        act[:, qw + ff:] = jnp.zeros((rows, pad), BF16)
        wod[qw + ff:, :] = jnp.zeros((pad, width), BF16)
    wait_input(0)
    for copy in weight_copies("od", 0):
        copy.start()
    for n in range(4):
        normalize(0, n, 4)
    for c in range(n_chunks):
        residual_copy(c).start()
    pl.semaphore_wait(barrier, 3)

    def step(i, carry):
        busy = i < total

        @pl.when(busy)
        def _():
            layer_start(i, "qkv")
            layer_start(i, "ff")
            expand(i)
            layer_end(i, "qkv")
            layer_end(i, "ff")
            for copy in kv_copies(i):
                copy.start()

            @pl.when(i + 1 < total)
            def _():
                start_input(i + 1)

        guarded(i - 4, gather_done)
        guarded(i - 2, second_done)
        guarded(i - 1, reduce_second)
        guarded(i - 2, gather_second)

        @pl.when(busy)
        def _():
            attention(i)
            for copy in kv_copies(i):
                copy.wait()

        guarded(i - 2, gather_forward)
        guarded(i - 3, gather_last)
        guarded(i - 1, first_done)

        @pl.when(busy)
        def _():
            layer_start(i, "od")

            @pl.when(i + 1 < total)
            def _():
                wait_input(i + 1)

            output(i, 0)

            @pl.when(i > 0)
            def _():
                pl.semaphore_wait(credit, 1)

            messages(i)(SIB).start()
            output(i, 1)
            layer_end(i, "od")

        guarded(i, reduce_first)
        guarded(i - 1, reduce_last)
        guarded(i - 3, gather_sibling)
        return carry

    lax.fori_loop(0, total + 4, step, 0)


def hand_over(*arrays):
    n_parts = (16, 2, 2)
    sizes = [a.shape[0] // n for a, n in zip(arrays, n_parts)]

    def kernel(*refs):
        n = len(arrays)
        ins, outs, bufs, sems = refs[:n], refs[n:2 * n], refs[2 * n:3 * n], refs[3 * n]
        reads, writes, count = [], [], 0
        for src, dst, buf, parts, size in zip(ins, outs, bufs, n_parts, sizes):
            for part_idx in range(parts):
                there = pl.ds(part_idx * size, size)
                reads.append(pltpu.make_async_copy(src.at[there], buf.at[part_idx], sems.at[0, count]))
                writes.append(pltpu.make_async_copy(buf.at[part_idx], dst.at[there], sems.at[1, count]))
                count += 1
        for copy in reads:
            copy.start()
        for read, write in zip(reads, writes):
            read.wait()
            write.start()
        for copy in writes:
            copy.wait()

    return pl.pallas_call(
        kernel,
        name="hand_over",
        out_shape=tuple(jax.ShapeDtypeStruct(a.shape, a.dtype) for a in arrays),
        in_specs=[pl.BlockSpec(memory_space=pl.ANY)] * len(arrays),
        out_specs=(pl.BlockSpec(memory_space=pl.ANY),) * len(arrays),
        scratch_shapes=[pltpu.VMEM((n, size) + a.shape[1:], a.dtype) for a, n, size in zip(arrays, n_parts, sizes)]
        + [pltpu.SemaphoreType.DMA((2, sum(n_parts)))],
        compiler_params=pltpu.CompilerParams(vmem_limit_bytes=60000000),
    )(*arrays)


def run_layers(x, positions, lengths, w_q, w_k, w_v, w_o, w_gate, w_up, w_down, norm_gain, q_gain, k_gain, n_tp):
    n_batch, seq, width = x.shape
    n_layers = w_q.shape[0]
    heads = w_q.shape[2] // HEAD_DIM
    ff = w_gate.shape[2]
    rows = min(CHUNK_ROWS, seq // 4)
    tokens = n_batch * seq
    n_chunks, per_seq, chips = tokens // rows, seq // rows, n_tp // 2
    quarter = rows // n_tp
    act_width = -(-(heads * HEAD_DIM + ff) // 256) * 256
    cfg = (n_layers, n_chunks, rows, per_seq, heads, chips)
    lane = np.arange(HEAD_DIM)
    freqs = np.stack([ROPE_THETA ** (-(lane // 2) * (2.0 / HEAD_DIM)), np.where(lane % 2 == 0, -1.0, 1.0)]).astype(np.float32)
    any_spec = pl.BlockSpec(memory_space=pl.ANY)
    vmem_spec = pl.BlockSpec(memory_space=pltpu.VMEM)
    dma = pltpu.SemaphoreType.DMA
    h, y, kc, vc = pl.pallas_call(
        functools.partial(layers_kernel, cfg),
        name="layers",
        out_shape=(
            jax.ShapeDtypeStruct((max(n_layers - 1, 1), tokens, width), BF16),
            jax.ShapeDtypeStruct((tokens, width), BF16),
            jax.ShapeDtypeStruct((n_layers, tokens, HEAD_DIM), BF16),
            jax.ShapeDtypeStruct((n_layers, tokens, HEAD_DIM), BF16),
        ),
        in_specs=[pl.BlockSpec(memory_space=pltpu.SMEM)] + [any_spec] * 8 + [vmem_spec] * 5,
        out_specs=(any_spec,) * 4,
        scratch_shapes=[
            pltpu.VMEM((width, (heads + 2) * HEAD_DIM), BF16),
            pltpu.VMEM((ff, width), BF16),
            pltpu.VMEM((ff, width), BF16),
            pltpu.VMEM((act_width, width), BF16),
            pltpu.VMEM((rows, width), BF16),
            pltpu.VMEM((rows, HEAD_DIM), F32),
            pltpu.VMEM((rows, HEAD_DIM), F32),
            pltpu.VMEM((rows, act_width), BF16),
            pltpu.VMEM((heads, rows, 2 * HEAD_DIM), BF16),
            pltpu.VMEM((seq, 2 * HEAD_DIM), BF16),
            pltpu.VMEM((seq, 2 * HEAD_DIM), BF16),
            pltpu.VMEM((heads, rows, HEAD_DIM), F32),
            pltpu.VMEM((heads, rows, 2 * HEAD_DIM), F32),
            pltpu.VMEM((rows, width), BF16),
            pltpu.VMEM((rows // 2, width), BF16),
            pltpu.VMEM((2, quarter, width // 2), BF16),
            pltpu.VMEM((2, quarter, width), F32),
            pltpu.VMEM((2, 2, quarter, width // 2), BF16),
            pltpu.VMEM((2, 2, quarter, width), BF16),
            pltpu.VMEM((AG_SLOTS, rows // 2, width), BF16),
            pltpu.VMEM((n_chunks, quarter, width), BF16),
            dma((7,)), dma((1,)), dma((2,)), dma((n_chunks,)), dma((AG_SLOTS,)), dma((N_MSG, AG_SLOTS)), dma((N_MSG, AG_SLOTS)),
            pltpu.SemaphoreType.REGULAR,
        ],
        compiler_params=pltpu.CompilerParams(collective_id=0, has_side_effects=True, vmem_limit_bytes=67043328),
    )(
        lengths, x.reshape(tokens, width), w_q, w_k, w_v, w_o, jnp.swapaxes(w_gate, 1, 2), jnp.swapaxes(w_up, 1, 2), w_down,
        positions.reshape(tokens // HEAD_DIM, HEAD_DIM), norm_gain, q_gain, k_gain, freqs
    )
    y, kc, vc = hand_over(y, kc.reshape(-1, HEAD_DIM), vc.reshape(-1, HEAD_DIM))
    y = y.reshape(n_batch, seq, width)
    cache_shape = (n_layers, n_batch, seq, 1, HEAD_DIM)
    return y, kc.reshape(cache_shape), vc.reshape(cache_shape)


def solution(mesh):
    act_spec = P('dp', None, None)
    col_spec = P(None, None, 'tp')
    row_spec = P(None, 'tp', None)
    cache_spec = P(None, 'dp', None, 'tp', None)
    in_specs = (act_spec, P('dp', None), P('dp'), col_spec, col_spec, col_spec, row_spec, col_spec, col_spec, row_spec, P(None, None), row_spec, row_spec)
    n_tp = mesh.shape['tp']

    def device_body(x, positions, lengths, w_q, w_k, w_v, w_o, w_gate, w_up, w_down, norm_gain, q_gain, k_gain):
        return run_layers(x, positions, lengths, w_q, w_k, w_v, w_o, w_gate, w_up, w_down, norm_gain, q_gain, k_gain, n_tp)

    return jax.shard_map(device_body, mesh=mesh, in_specs=in_specs, out_specs=(act_spec, cache_spec, cache_spec), check_vma=False)
```

```python
import functools

import jax
import jax.numpy as jnp
import numpy as np
from jax import lax
from jax.experimental import pallas as pl
from jax.experimental.pallas import tpu as pltpu
from jax.sharding import PartitionSpec as P

HEAD_DIM = 128
ROPE_THETA = 75000000.0
NORM_EPS = 1e-5
NEG = -1e30
LOG2E = 1.4426950408889634
CHUNK_ROWS = 512
AG_SLOTS = 3
MESH = pl.DeviceIdType.MESH
F32 = jnp.float32
BF16 = jnp.bfloat16

SIB, M1L, M1R, M2L, M2R, M3L, M3R, A1L, A1R, A2L, A2R, A3L, A3R, AS = range(14)
N_MSG = 17


def mm(a, b):
    return jnp.dot(a, b, preferred_element_type=F32)


def mm_t(a, b):
    return lax.dot_general(a, b, (((1,), (1,)), ((), ())), preferred_element_type=F32)


def norm_last(values, gain):
    width = values.shape[-1]
    mean = jnp.sum(values, axis=-1, keepdims=True) * (1.0 / width)
    centered = values - mean
    var = jnp.sum(centered * centered, axis=-1, keepdims=True) * (1.0 / width)
    return centered * lax.rsqrt(var + NORM_EPS) * gain


def cos_sin(angles):
    turns = jnp.round(angles * 0.6366197723675814)
    r = ((angles - turns * 1.5703125) - turns * 4.837512969970703e-4) - turns * 7.549789954891882e-8
    r2 = r * r
    sin_r = r + r * r2 * (-1.6666654611e-1 + r2 * (8.3321608736e-3 - r2 * 1.9515295891e-4))
    cos_r = 1.0 - 0.5 * r2 + r2 * r2 * (4.166664568298827e-2 + r2 * (-1.388731625493765e-3 + r2 * 2.443315711809948e-5))
    quad = turns.astype(jnp.int32) & 3
    odd = (quad & 1) == 1
    cos = jnp.where(odd, sin_r, cos_r)
    sin = jnp.where(odd, cos_r, sin_r)
    cos = jnp.where((quad == 1) | (quad == 2), -cos, cos)
    sin = jnp.where(quad >= 2, -sin, sin)
    return cos, sin


def rope(values, cos, sin):
    lane = lax.broadcasted_iota(jnp.int32, values.shape, 1)
    swapped = jnp.where(lane % 2 == 0, pltpu.roll(values, HEAD_DIM - 1, 1), pltpu.roll(values, 1, 1))
    return values * cos + swapped * sin


def layers_kernel(
    cfg,
    len_ref, x_ref, wq_ref, wk_ref, wv_ref, wo_ref, wg_ref, wu_ref, wd_ref, pos_ref, ng_ref, qg_ref, kg_ref, fr_ref,
    h_ref, y_ref, kc_ref, vc_ref,
    wqkv, wg, wu, wod, xn, cs, sn, act, q_scr, k_scr, v_scr, m_scr, acc_scr, part, rsib, m3, own, ro, rf, ag, hres,
    w_sem, in_sem, kv_sem, res_sem, ago_sem, s_sem, r_sem, credit,
):
    n_layers, n_chunks, rows, per_seq, heads, chips = cfg
    width = x_ref.shape[1]
    half = width // 2
    ff = wg_ref.shape[1]
    qw = heads * HEAD_DIM
    quarter = rows // (2 * chips)
    hrows = rows // 2
    total = n_layers * n_chunks
    c_exp = HEAD_DIM ** -0.5 * LOG2E

    me = lax.axis_index("tp")
    chip, core = me // 2, me % 2
    left_chip, right_chip, far_chip = (chip + chips - 1) % chips, (chip + 1) % chips, (chip + 2) % chips
    left, right, sib = left_chip * 2 + core, right_chip * 2 + core, chip * 2 + 1 - core
    my_base, sib_base = core * hrows, (1 - core) * hrows

    def block(chip_id):
        return pl.ds(pl.multiple_of(my_base + chip_id * quarter, quarter), quarter)

    def sub(chip_id):
        return pl.ds(pl.multiple_of(chip_id * quarter, quarter), quarter)

    my_half = pl.ds(pl.multiple_of(my_base, hrows), hrows)
    sib_half = pl.ds(pl.multiple_of(sib_base, hrows), hrows)
    first, second = pl.ds(0, half), pl.ds(half, half)

    def msg(kind, slot, src, dst, dev):
        return pltpu.make_async_remote_copy(
            src_ref=src, dst_ref=dst, send_sem=s_sem.at[kind, slot], recv_sem=r_sem.at[kind, slot],
            device_id={"tp": dev}, device_id_type=MESH,
        )

    def messages(g):
        slot = g % 2
        p, a = part, ag.at[g % AG_SLOTS]
        lb, rb, fb = block(left_chip), block(right_chip), block(far_chip)
        mine, from_left, from_right = sub(chip), sub(left_chip), sub(right_chip)
        table = {
            SIB: (p.at[sib_half], rsib, sib),
            M1L: (p.at[fb, first], ro.at[slot, 0], left),
            M1R: (p.at[fb, second], ro.at[slot, 1], right),
            M2L: (p.at[lb, second], rf.at[slot, 0, :, second], left),
            M2R: (p.at[rb, first], rf.at[slot, 1, :, first], right),
            M3L: (m3.at[0], rf.at[slot, 0, :, first], left),
            M3R: (m3.at[1], rf.at[slot, 1, :, second], right),
            A1L: (a.at[mine, first], a.at[mine, first], left),
            A1R: (a.at[mine, second], a.at[mine, second], right),
            A2L: (a.at[mine, second], a.at[mine, second], left),
            A2R: (a.at[mine, first], a.at[mine, first], right),
            A3L: (a.at[from_right, first], a.at[from_right, first], left),
            A3R: (a.at[from_left, second], a.at[from_left, second], right),
        }
        return lambda kind: msg(kind, g % AG_SLOTS if kind >= A1L else slot, *table[kind])

    def chunk_rows(g):
        return pl.ds(pl.multiple_of((g % n_chunks) * rows, rows), rows)

    def weight_copies(which, layer):
        groups = {
            "qkv": [
                (wq_ref.at[layer], wqkv.at[:, pl.ds(0, qw)], 0),
                (wk_ref.at[layer], wqkv.at[:, pl.ds(qw, HEAD_DIM)], 1),
                (wv_ref.at[layer], wqkv.at[:, pl.ds(qw + HEAD_DIM, HEAD_DIM)], 2),
            ],
            "ff": [(wg_ref.at[layer], wg, 3), (wu_ref.at[layer], wu, 4)],
            "od": [(wo_ref.at[layer], wod.at[pl.ds(0, qw)], 5), (wd_ref.at[layer], wod.at[pl.ds(qw, ff)], 6)],
        }
        return [pltpu.make_async_copy(src, dst, w_sem.at[n]) for src, dst, n in groups[which]]

    def start_input(g):
        r = chunk_rows(g)

        @pl.when(g < n_chunks)
        def _():
            pltpu.make_async_copy(x_ref.at[r], xn, in_sem.at[0]).start()

        @pl.when(g >= n_chunks)
        def _():
            pltpu.make_async_copy(h_ref.at[g // n_chunks - 1, r], xn, in_sem.at[0]).start()

    def wait_input(g):
        pltpu.make_async_copy(x_ref.at[chunk_rows(g)], xn, in_sem.at[0]).wait()

    def seq_start(g):
        return pl.multiple_of((g % per_seq) * rows, rows)

    def kv_copies(g):
        here = pl.ds(seq_start(g), rows)
        r = chunk_rows(g)
        return [
            pltpu.make_async_copy(k_scr.at[here, pl.ds(0, HEAD_DIM)], kc_ref.at[g // n_chunks, r], kv_sem.at[0]),
            pltpu.make_async_copy(v_scr.at[here, pl.ds(0, HEAD_DIM)], vc_ref.at[g // n_chunks, r], kv_sem.at[1]),
        ]

    def gathered(g):
        slot = g % AG_SLOTS
        src = ag.at[slot]
        base = (g % n_chunks) * rows + my_base
        last = g >= total - n_chunks

        def to_mine(ref):
            return pltpu.make_async_copy(src, ref.at[pl.ds(pl.multiple_of(base, hrows), hrows)], ago_sem.at[slot])

        def to_sibling(ref, n):
            chip_id = (chip, left_chip, right_chip, far_chip)[n]
            dst = ref.at[pl.ds(pl.multiple_of(base + chip_id * quarter, quarter), quarter)]
            return msg(AS + n, slot, src.at[sub(chip_id)], dst, sib)

        def start(blocks, mine):
            def into(ref):
                for n in blocks:
                    to_sibling(ref, n).start()
                if mine:
                    to_mine(ref).start()

            @pl.when(last)
            def _():
                into(y_ref)

            @pl.when(jnp.logical_not(last))
            def _():
                into(h_ref.at[g // n_chunks])

        return start, to_mine, to_sibling

    def residual_copy(c):
        src = pl.ds(pl.multiple_of(c * rows + my_base + chip * quarter, quarter), quarter)
        return pltpu.make_async_copy(x_ref.at[src], hres.at[c], res_sem.at[c])

    def reduce_first(g):
        slot = g % 2
        m = messages(g)
        m(SIB).wait_recv()
        p, s = part, rsib

        def fold(chip_id):
            b = block(chip_id)
            p[b, :] = (p[b, :].astype(F32) + s[sub(chip_id), :].astype(F32)).astype(BF16)

        fold(far_chip)
        m(M1L).start()
        m(M1R).start()
        fold(left_chip)
        m(M2L).start()
        fold(right_chip)
        m(M2R).start()
        own[slot] = p[block(chip), :].astype(F32) + s[sub(chip), :].astype(F32)

        @pl.when(g < total - 1)
        def _():
            pl.semaphore_signal(credit, inc=1, device_id={"tp": sib}, device_id_type=MESH)

    def reduce_second(g):
        slot = g % 2
        m = messages(g)
        m(M1L).wait_recv()
        m3[0] = (part[block(left_chip), first].astype(F32) + ro[slot, 0].astype(F32)).astype(BF16)
        m(M3L).start()
        m(M1R).wait_recv()
        m3[1] = (part[block(right_chip), second].astype(F32) + ro[slot, 1].astype(F32)).astype(BF16)
        m(M3R).start()

    def reduce_last(g):
        slot = g % 2
        c = g % n_chunks
        m = messages(g)
        for kind in (M2L, M2R, M3L, M3R):
            m(kind).wait_recv()

        @pl.when(g < n_chunks)
        def _():
            residual_copy(c).wait()

        h = (own[slot] + (rf[slot, 0].astype(F32) + rf[slot, 1].astype(F32)) + hres[c].astype(F32)).astype(BF16)
        hres[c] = h
        ag[g % AG_SLOTS, sub(chip), :] = h
        for kind in (A1L, A1R):
            m(kind).start()

    def gather_second(g):
        m = messages(g)
        for kind in (A2L, A2R):
            m(kind).start()

    def gather_forward(g):
        m = messages(g)
        m(A1L).wait_recv()
        m(A3L).start()
        m(A1R).wait_recv()
        m(A3R).start()

    def gather_last(g):
        slot = g % 2
        m = messages(g)
        start = gathered(g)[0]
        for kind in (A2L, A2R):
            m(kind).wait_recv()
        start((0, 1, 2), False)
        for kind in (A3L, A3R):
            m(kind).wait_recv()
        start((3,), True)

    def gather_sibling(g):
        for n in range(4):
            gathered(g)[2](y_ref, n).wait_recv()

    def gather_done(g):
        m = messages(g)
        for kind in (A1L, A1R, A2L, A2R, A3L, A3R):
            m(kind).wait_send()
        _, to_mine, to_sibling = gathered(g)
        to_mine(y_ref).wait()
        for n in range(4):
            to_sibling(y_ref, n).wait_send()

    def first_done(g):
        m = messages(g)
        for kind in (SIB, M1L, M1R, M2L, M2R):
            m(kind).wait_send()

    def second_done(g):
        m = messages(g)
        for kind in (M3L, M3R):
            m(kind).wait_send()

    def guarded(g, fn):
        @pl.when(jnp.logical_and(g >= 0, g < total))
        def _():
            fn(g)

    def normalize(g, part_idx, n_parts):
        size = rows // n_parts
        rr = pl.ds(part_idx * size, size)
        gain = ng_ref[pl.ds(jnp.minimum(g // n_chunks, n_layers - 1), 1), :]
        xn[rr, :] = norm_last(xn[rr, :].astype(F32), gain).astype(BF16)

    def expand(g):
        n = xn[...]
        layer = g // n_chunks
        here = pl.ds(seq_start(g), rows)
        for n_row in range(rows // HEAD_DIM):
            tokens_here = pl.ds(pl.multiple_of(seq_start(g) + n_row * HEAD_DIM, HEAD_DIM), HEAD_DIM)
            both = pos_ref[:, tokens_here].astype(F32)
            wanted = lax.broadcasted_iota(jnp.int32, both.shape, 0) == (g % n_chunks) // per_seq
            row = jnp.sum(jnp.where(wanted, both, 0.0), axis=0, keepdims=True)
            down = jnp.transpose(jnp.broadcast_to(row, (HEAD_DIM, HEAD_DIM)))
            cos, sin = cos_sin(down * fr_ref[0:1, :])
            part_rows = slice(n_row * HEAD_DIM, (n_row + 1) * HEAD_DIM)
            cs[part_rows, :] = cos
            sn[part_rows, :] = sin * fr_ref[1:2, :]

        def head(values, gain):
            return rope(norm_last(values, gain), cs[...], sn[...]).astype(BF16)

        def put_k(values):
            k_scr[here, :HEAD_DIM] = head(values, kg_ref[layer])

        def put_q(hd):
            def put(values):
                q_scr[hd, :, :HEAD_DIM] = head(values, qg_ref[layer, hd:hd + 1, :])
            return put

        z = mm(n, wqkv[:, qw:qw + 2 * HEAD_DIM])
        v_scr[here, :HEAD_DIM] = z[:, HEAD_DIM:].astype(BF16)
        pending = [(put_k, z[:, :HEAD_DIM])]
        row_id = seq_start(g) + lax.broadcasted_iota(jnp.int32, (rows, HEAD_DIM), 0)
        lane = lax.broadcasted_iota(jnp.int32, (rows, HEAD_DIM), 1)
        length = len_ref[(g % n_chunks) // per_seq]
        k_scr[here, HEAD_DIM:] = jnp.where(jnp.logical_and(lane == 0, row_id >= length), NEG, 0.0).astype(BF16)
        for pair in range(heads // 2):
            z = mm(n, wqkv[:, pair * 2 * HEAD_DIM:(pair + 1) * 2 * HEAD_DIM])
            pending += [(put_q(2 * pair + e), z[:, e * HEAD_DIM:(e + 1) * HEAD_DIM]) for e in range(2)]
        for c0 in range(0, ff, 256):
            c1 = min(c0 + 256, ff)
            gate = mm_t(n, wg[c0:c1, :])
            up = mm_t(n, wu[c0:c1, :])
            if pending:
                put, values = pending.pop(0)
                put(values)
            act[:, qw + c0:qw + c1] = (jax.nn.silu(gate) * up).astype(BF16)
        for put, values in pending:
            put(values)

    def attention(g):
        s0 = seq_start(g)
        lanes = HEAD_DIM
        size = min(rows, 256)

        def stream(units, scores, soft, weigh):
            following, last = scores(units[0]), None
            for n, unit in enumerate(units):
                current = following
                if n + 1 < len(units):
                    following = scores(units[n + 1])
                probs = soft(unit, current)
                if last is not None:
                    weigh(*last)
                last = (unit, probs)
            weigh(*last)

        def top_of(tiles):
            top = tiles[0]
            for t in tiles[1:]:
                top = jnp.maximum(top, t)
            return jnp.max(top, axis=-1, keepdims=True)

        def probs_of(tiles, top):
            return jnp.concatenate([jnp.exp2((t - top) * c_exp).astype(BF16) for t in tiles], axis=1)

        step = 2 * size
        n_units = rows // size
        offset = lax.broadcasted_iota(jnp.int32, (size, lanes), 0) - lax.broadcasted_iota(jnp.int32, (size, lanes), 1)

        def own(first_half):
            base = pl.multiple_of(s0 - first_half * size, size)

            def own_keys(n):
                return pl.ds(base, (first_half + n + 1) * size)

            def own_scores(unit):
                hd, n = unit
                return mm_t(q_scr[hd, n * size:(n + 1) * size, :], k_scr[own_keys(n), :])

            def own_soft(unit, s):
                hd, n = unit
                before = (first_half + n) * size
                tiles = []
                for t in range(0, before + size, lanes):
                    tile = s[:, t:t + lanes]
                    tiles.append(tile if t < before else jnp.where(offset >= t - before, tile, NEG))
                top = top_of(tiles)
                m_scr[hd, n * size:(n + 1) * size, :] = jnp.broadcast_to(top, (size, lanes))
                return probs_of(tiles, top)

            def own_weigh(unit, p):
                hd, n = unit
                acc_scr[hd, n * size:(n + 1) * size, :] = mm(p, v_scr[own_keys(n), :])

            stream([(hd, n) for hd in range(heads) for n in range(n_units)], own_scores, own_soft, own_weigh)

        if n_units == 2:
            own(0)
        else:
            for odd in range(2):
                @pl.when((s0 // size) % 2 == odd)
                def _():
                    own(odd)

        def body(j, carry):
            keys = pl.ds(pl.multiple_of(j * step, step), step)

            def scores(hd):
                return mm_t(q_scr[hd], k_scr[keys, :])

            def soft(hd, s):
                tiles = [s[:, t:t + lanes] for t in range(0, step, lanes)]
                old = m_scr[hd]
                top = jnp.maximum(old, top_of(tiles))
                m_scr[hd] = top
                return probs_of(tiles, top), jnp.exp2((old - top) * c_exp)

            def weigh(hd, probs):
                p, scale = probs
                pv = mm(p, v_scr[keys, :])
                acc_scr[hd, :, :lanes] = acc_scr[hd, :, :lanes] * scale + pv[:, :lanes]
                acc_scr[hd, :, lanes:] = acc_scr[hd, :, lanes:] * scale + pv[:, lanes:]

            stream(list(range(heads)), scores, soft, weigh)
            return carry

        lax.fori_loop(0, s0 // step, body, 0)
        for hd in range(heads):
            out = acc_scr[hd, :, :lanes] / acc_scr[hd, :, lanes:]
            act[:, hd * lanes:(hd + 1) * lanes] = out.astype(BF16)

    def output(g, side):
        p = part
        r = (sib_half, my_half)[side]
        a = act[r, :]
        n_cols = 2
        step = width // n_cols
        for n in range(n_cols):
            p[r, n * step:(n + 1) * step] = mm(a, wod[:, n * step:(n + 1) * step]).astype(BF16)
            normalize(g + 1, 2 * side + n, 4)

    def layer_start(g, which):
        @pl.when(g % n_chunks == 0)
        def _():
            for copy in weight_copies(which, g // n_chunks):
                copy.wait()

    def layer_end(g, which):
        @pl.when(jnp.logical_and(g % n_chunks == n_chunks - 1, g < total - 1))
        def _():
            for copy in weight_copies(which, g // n_chunks + 1):
                copy.start()

    start_input(0)
    for copy in weight_copies("qkv", 0) + weight_copies("ff", 0):
        copy.start()
    barrier = pltpu.get_barrier_semaphore()
    for dev in (left, right, sib):
        pl.semaphore_signal(barrier, inc=1, device_id={"tp": dev}, device_id_type=MESH)
    q_scr[:, :, HEAD_DIM:] = jnp.ones((heads, rows, HEAD_DIM), BF16)
    v_scr[:, HEAD_DIM:] = jnp.ones((v_scr.shape[0], HEAD_DIM), BF16)
    pad = act.shape[1] - (qw + ff)
    if pad:
        act[:, qw + ff:] = jnp.zeros((rows, pad), BF16)
        wod[qw + ff:, :] = jnp.zeros((pad, width), BF16)
    wait_input(0)
    for copy in weight_copies("od", 0):
        copy.start()
    for n in range(4):
        normalize(0, n, 4)
    for c in range(n_chunks):
        residual_copy(c).start()
    pl.semaphore_wait(barrier, 3)

    def step(i, carry):
        busy = i < total

        @pl.when(busy)
        def _():
            layer_start(i, "qkv")
            layer_start(i, "ff")
            expand(i)
            layer_end(i, "qkv")
            layer_end(i, "ff")
            for copy in kv_copies(i):
                copy.start()

            @pl.when(i + 1 < total)
            def _():
                start_input(i + 1)

        guarded(i - 4, gather_done)
        guarded(i - 2, second_done)
        guarded(i - 1, reduce_second)
        guarded(i - 2, gather_second)

        @pl.when(busy)
        def _():
            attention(i)
            for copy in kv_copies(i):
                copy.wait()

        guarded(i - 2, gather_forward)
        guarded(i - 3, gather_last)
        guarded(i - 1, first_done)

        @pl.when(busy)
        def _():
            layer_start(i, "od")

            @pl.when(i + 1 < total)
            def _():
                wait_input(i + 1)

            output(i, 0)

            @pl.when(i > 0)
            def _():
                pl.semaphore_wait(credit, 1)

            messages(i)(SIB).start()
            output(i, 1)
            layer_end(i, "od")

        guarded(i, reduce_first)
        guarded(i - 1, reduce_last)
        guarded(i - 3, gather_sibling)
        return carry

    lax.fori_loop(0, total + 4, step, 0)


def hand_over(*arrays):
    n_parts = (16, 2, 2)
    sizes = [a.shape[0] // n for a, n in zip(arrays, n_parts)]

    def kernel(*refs):
        n = len(arrays)
        ins, outs, bufs, sems = refs[:n], refs[n:2 * n], refs[2 * n:3 * n], refs[3 * n]
        reads, writes, count = [], [], 0
        for src, dst, buf, parts, size in zip(ins, outs, bufs, n_parts, sizes):
            for part_idx in range(parts):
                there = pl.ds(part_idx * size, size)
                reads.append(pltpu.make_async_copy(src.at[there], buf.at[part_idx], sems.at[0, count]))
                writes.append(pltpu.make_async_copy(buf.at[part_idx], dst.at[there], sems.at[1, count]))
                count += 1
        for copy in reads:
            copy.start()
        for read, write in zip(reads, writes):
            read.wait()
            write.start()
        for copy in writes:
            copy.wait()

    return pl.pallas_call(
        kernel,
        name="hand_over",
        out_shape=tuple(jax.ShapeDtypeStruct(a.shape, a.dtype) for a in arrays),
        in_specs=[pl.BlockSpec(memory_space=pl.ANY)] * len(arrays),
        out_specs=(pl.BlockSpec(memory_space=pl.ANY),) * len(arrays),
        scratch_shapes=[pltpu.VMEM((n, size) + a.shape[1:], a.dtype) for a, n, size in zip(arrays, n_parts, sizes)]
        + [pltpu.SemaphoreType.DMA((2, sum(n_parts)))],
        compiler_params=pltpu.CompilerParams(vmem_limit_bytes=60000000),
    )(*arrays)


def run_layers(x, positions, lengths, w_q, w_k, w_v, w_o, w_gate, w_up, w_down, norm_gain, q_gain, k_gain, n_tp):
    n_batch, seq, width = x.shape
    n_layers = w_q.shape[0]
    heads = w_q.shape[2] // HEAD_DIM
    ff = w_gate.shape[2]
    rows = min(CHUNK_ROWS, seq // 4)
    tokens = n_batch * seq
    n_chunks, per_seq, chips = tokens // rows, seq // rows, n_tp // 2
    quarter = rows // n_tp
    act_width = -(-(heads * HEAD_DIM + ff) // 256) * 256
    cfg = (n_layers, n_chunks, rows, per_seq, heads, chips)
    lane = np.arange(HEAD_DIM)
    freqs = np.stack([ROPE_THETA ** (-(lane // 2) * (2.0 / HEAD_DIM)), np.where(lane % 2 == 0, -1.0, 1.0)]).astype(np.float32)
    any_spec = pl.BlockSpec(memory_space=pl.ANY)
    vmem_spec = pl.BlockSpec(memory_space=pltpu.VMEM)
    dma = pltpu.SemaphoreType.DMA
    h, y, kc, vc = pl.pallas_call(
        functools.partial(layers_kernel, cfg),
        name="layers",
        out_shape=(
            jax.ShapeDtypeStruct((max(n_layers - 1, 1), tokens, width), BF16),
            jax.ShapeDtypeStruct((tokens, width), BF16),
            jax.ShapeDtypeStruct((n_layers, tokens, HEAD_DIM), BF16),
            jax.ShapeDtypeStruct((n_layers, tokens, HEAD_DIM), BF16),
        ),
        in_specs=[pl.BlockSpec(memory_space=pltpu.SMEM)] + [any_spec] * 8 + [vmem_spec] * 5,
        out_specs=(any_spec,) * 4,
        scratch_shapes=[
            pltpu.VMEM((width, (heads + 2) * HEAD_DIM), BF16),
            pltpu.VMEM((ff, width), BF16),
            pltpu.VMEM((ff, width), BF16),
            pltpu.VMEM((act_width, width), BF16),
            pltpu.VMEM((rows, width), BF16),
            pltpu.VMEM((rows, HEAD_DIM), F32),
            pltpu.VMEM((rows, HEAD_DIM), F32),
            pltpu.VMEM((rows, act_width), BF16),
            pltpu.VMEM((heads, rows, 2 * HEAD_DIM), BF16),
            pltpu.VMEM((seq, 2 * HEAD_DIM), BF16),
            pltpu.VMEM((seq, 2 * HEAD_DIM), BF16),
            pltpu.VMEM((heads, rows, HEAD_DIM), F32),
            pltpu.VMEM((heads, rows, 2 * HEAD_DIM), F32),
            pltpu.VMEM((rows, width), BF16),
            pltpu.VMEM((rows // 2, width), BF16),
            pltpu.VMEM((2, quarter, width // 2), BF16),
            pltpu.VMEM((2, quarter, width), F32),
            pltpu.VMEM((2, 2, quarter, width // 2), BF16),
            pltpu.VMEM((2, 2, quarter, width), BF16),
            pltpu.VMEM((AG_SLOTS, rows // 2, width), BF16),
            pltpu.VMEM((n_chunks, quarter, width), BF16),
            dma((7,)), dma((1,)), dma((2,)), dma((n_chunks,)), dma((AG_SLOTS,)), dma((N_MSG, AG_SLOTS)), dma((N_MSG, AG_SLOTS)),
            pltpu.SemaphoreType.REGULAR,
        ],
        compiler_params=pltpu.CompilerParams(collective_id=0, has_side_effects=True, vmem_limit_bytes=67043328),
    )(
        lengths, x.reshape(tokens, width), w_q, w_k, w_v, w_o, jnp.swapaxes(w_gate, 1, 2), jnp.swapaxes(w_up, 1, 2), w_down,
        positions, norm_gain, q_gain, k_gain, freqs
    )
    y, kc, vc = hand_over(y, kc.reshape(-1, HEAD_DIM), vc.reshape(-1, HEAD_DIM))
    y = y.reshape(n_batch, seq, width)
    cache_shape = (n_layers, n_batch, seq, 1, HEAD_DIM)
    return y, kc.reshape(cache_shape), vc.reshape(cache_shape)


def solution(mesh):
    act_spec = P('dp', None, None)
    col_spec = P(None, None, 'tp')
    row_spec = P(None, 'tp', None)
    cache_spec = P(None, 'dp', None, 'tp', None)
    in_specs = (act_spec, P('dp', None), P('dp'), col_spec, col_spec, col_spec, row_spec, col_spec, col_spec, row_spec, P(None, None), row_spec, row_spec)
    n_tp = mesh.shape['tp']

    def device_body(x, positions, lengths, w_q, w_k, w_v, w_o, w_gate, w_up, w_down, norm_gain, q_gain, k_gain):
        return run_layers(x, positions, lengths, w_q, w_k, w_v, w_o, w_gate, w_up, w_down, norm_gain, q_gain, k_gain, n_tp)

    return jax.shard_map(device_body, mesh=mesh, in_specs=in_specs, out_specs=(act_spec, cache_spec, cache_spec), check_vma=False)
```

```python
import functools

import jax
import jax.numpy as jnp
import numpy as np
from jax import lax
from jax.experimental import pallas as pl
from jax.experimental.pallas import tpu as pltpu
from jax.sharding import PartitionSpec as P

HEAD_DIM = 128
ROPE_THETA = 75000000.0
NORM_EPS = 1e-5
NEG = -1e30
LOG2E = 1.4426950408889634
CHUNK_ROWS = 512
AG_SLOTS = 3
MESH = pl.DeviceIdType.MESH
F32 = jnp.float32
BF16 = jnp.bfloat16

SIB, M1L, M1R, M2L, M2R, M3L, M3R, A1L, A1R, A2L, A2R, A3L, A3R, AS = range(14)
N_MSG = 17


def mm(a, b):
    return jnp.dot(a, b, preferred_element_type=F32)


def mm_t(a, b):
    return lax.dot_general(a, b, (((1,), (1,)), ((), ())), preferred_element_type=F32)


def norm_last(values, gain):
    width = values.shape[-1]
    mean = jnp.sum(values, axis=-1, keepdims=True) * (1.0 / width)
    centered = values - mean
    var = jnp.sum(centered * centered, axis=-1, keepdims=True) * (1.0 / width)
    return centered * lax.rsqrt(var + NORM_EPS) * gain


def cos_sin(angles):
    turns = jnp.round(angles * 0.6366197723675814)
    r = ((angles - turns * 1.5703125) - turns * 4.837512969970703e-4) - turns * 7.549789954891882e-8
    r2 = r * r
    sin_r = r + r * r2 * (-1.6666654611e-1 + r2 * (8.3321608736e-3 - r2 * 1.9515295891e-4))
    cos_r = 1.0 - 0.5 * r2 + r2 * r2 * (4.166664568298827e-2 + r2 * (-1.388731625493765e-3 + r2 * 2.443315711809948e-5))
    quad = turns.astype(jnp.int32) & 3
    odd = (quad & 1) == 1
    cos = jnp.where(odd, sin_r, cos_r)
    sin = jnp.where(odd, cos_r, sin_r)
    cos = jnp.where((quad == 1) | (quad == 2), -cos, cos)
    sin = jnp.where(quad >= 2, -sin, sin)
    return cos, sin


def rope(values, cos, sin):
    lane = lax.broadcasted_iota(jnp.int32, values.shape, 1)
    swapped = jnp.where(lane % 2 == 0, pltpu.roll(values, HEAD_DIM - 1, 1), pltpu.roll(values, 1, 1))
    return values * cos + swapped * sin


def layers_kernel(
    cfg,
    len_ref, x_ref, wq_ref, wk_ref, wv_ref, wo_ref, wg_ref, wu_ref, wd_ref, pos_ref, ng_ref, qg_ref, kg_ref, fr_ref,
    h_ref, y_ref, kc_ref, vc_ref,
    wqkv, wg, wu, wod, xn, cs, sn, act, q_scr, k_scr, v_scr, m_scr, acc_scr, part, rsib, m3, own, ro, rf, ag, hres,
    w_sem, in_sem, kv_sem, res_sem, ago_sem, s_sem, r_sem, credit,
):
    n_layers, n_chunks, rows, per_seq, heads, chips = cfg
    width = x_ref.shape[1]
    half = width // 2
    ff = wg_ref.shape[1]
    qw = heads * HEAD_DIM
    quarter = rows // (2 * chips)
    hrows = rows // 2
    total = n_layers * n_chunks
    c_exp = HEAD_DIM ** -0.5 * LOG2E

    me = lax.axis_index("tp")
    chip, core = me // 2, me % 2
    left_chip, right_chip, far_chip = (chip + chips - 1) % chips, (chip + 1) % chips, (chip + 2) % chips
    left, right, sib = left_chip * 2 + core, right_chip * 2 + core, chip * 2 + 1 - core
    my_base, sib_base = core * hrows, (1 - core) * hrows

    def block(chip_id):
        return pl.ds(pl.multiple_of(my_base + chip_id * quarter, quarter), quarter)

    def sub(chip_id):
        return pl.ds(pl.multiple_of(chip_id * quarter, quarter), quarter)

    my_half = pl.ds(pl.multiple_of(my_base, hrows), hrows)
    sib_half = pl.ds(pl.multiple_of(sib_base, hrows), hrows)
    first, second = pl.ds(0, half), pl.ds(half, half)

    def msg(kind, slot, src, dst, dev):
        return pltpu.make_async_remote_copy(
            src_ref=src, dst_ref=dst, send_sem=s_sem.at[kind, slot], recv_sem=r_sem.at[kind, slot],
            device_id={"tp": dev}, device_id_type=MESH,
        )

    def messages(g):
        slot = g % 2
        p, a = part, ag.at[g % AG_SLOTS]
        lb, rb, fb = block(left_chip), block(right_chip), block(far_chip)
        mine, from_left, from_right = sub(chip), sub(left_chip), sub(right_chip)
        table = {
            SIB: (p.at[sib_half], rsib, sib),
            M1L: (p.at[fb, first], ro.at[slot, 0], left),
            M1R: (p.at[fb, second], ro.at[slot, 1], right),
            M2L: (p.at[lb, second], rf.at[slot, 0, :, second], left),
            M2R: (p.at[rb, first], rf.at[slot, 1, :, first], right),
            M3L: (m3.at[0], rf.at[slot, 0, :, first], left),
            M3R: (m3.at[1], rf.at[slot, 1, :, second], right),
            A1L: (a.at[mine, first], a.at[mine, first], left),
            A1R: (a.at[mine, second], a.at[mine, second], right),
            A2L: (a.at[mine, second], a.at[mine, second], left),
            A2R: (a.at[mine, first], a.at[mine, first], right),
            A3L: (a.at[from_right, first], a.at[from_right, first], left),
            A3R: (a.at[from_left, second], a.at[from_left, second], right),
        }
        return lambda kind: msg(kind, g % AG_SLOTS if kind >= A1L else slot, *table[kind])

    def chunk_rows(g):
        return pl.ds(pl.multiple_of((g % n_chunks) * rows, rows), rows)

    def weight_copies(which, layer):
        groups = {
            "qkv": [
                (wq_ref.at[layer], wqkv.at[:, pl.ds(0, qw)], 0),
                (wk_ref.at[layer], wqkv.at[:, pl.ds(qw, HEAD_DIM)], 1),
                (wv_ref.at[layer], wqkv.at[:, pl.ds(qw + HEAD_DIM, HEAD_DIM)], 2),
            ],
            "ff": [(wg_ref.at[layer], wg, 3), (wu_ref.at[layer], wu, 4)],
            "od": [(wo_ref.at[layer], wod.at[pl.ds(0, qw)], 5), (wd_ref.at[layer], wod.at[pl.ds(qw, ff)], 6)],
        }
        return [pltpu.make_async_copy(src, dst, w_sem.at[n]) for src, dst, n in groups[which]]

    def start_input(g):
        r = chunk_rows(g)

        @pl.when(g < n_chunks)
        def _():
            pltpu.make_async_copy(x_ref.at[r], xn, in_sem.at[0]).start()

        @pl.when(g >= n_chunks)
        def _():
            pltpu.make_async_copy(h_ref.at[g // n_chunks - 1, r], xn, in_sem.at[0]).start()

    def wait_input(g):
        pltpu.make_async_copy(x_ref.at[chunk_rows(g)], xn, in_sem.at[0]).wait()

    def seq_start(g):
        return pl.multiple_of((g % per_seq) * rows, rows)

    def kv_copies(g):
        here = pl.ds(seq_start(g), rows)
        r = chunk_rows(g)
        return [
            pltpu.make_async_copy(k_scr.at[here, pl.ds(0, HEAD_DIM)], kc_ref.at[g // n_chunks, r], kv_sem.at[0]),
            pltpu.make_async_copy(v_scr.at[here, pl.ds(0, HEAD_DIM)], vc_ref.at[g // n_chunks, r], kv_sem.at[1]),
        ]

    def gathered(g):
        slot = g % AG_SLOTS
        src = ag.at[slot]
        base = (g % n_chunks) * rows + my_base
        last = g >= total - n_chunks

        def to_mine(ref):
            return pltpu.make_async_copy(src, ref.at[pl.ds(pl.multiple_of(base, hrows), hrows)], ago_sem.at[slot])

        def to_sibling(ref, n):
            chip_id = (chip, left_chip, right_chip, far_chip)[n]
            dst = ref.at[pl.ds(pl.multiple_of(base + chip_id * quarter, quarter), quarter)]
            return msg(AS + n, slot, src.at[sub(chip_id)], dst, sib)

        def start(blocks, mine):
            def into(ref):
                for n in blocks:
                    to_sibling(ref, n).start()
                if mine:
                    to_mine(ref).start()

            @pl.when(last)
            def _():
                into(y_ref)

            @pl.when(jnp.logical_not(last))
            def _():
                into(h_ref.at[g // n_chunks])

        return start, to_mine, to_sibling

    def residual_copy(c):
        src = pl.ds(pl.multiple_of(c * rows + my_base + chip * quarter, quarter), quarter)
        return pltpu.make_async_copy(x_ref.at[src], hres.at[c], res_sem.at[c])

    def reduce_first(g):
        slot = g % 2
        m = messages(g)
        m(SIB).wait_recv()
        p, s = part, rsib

        def fold(chip_id):
            b = block(chip_id)
            p[b, :] = (p[b, :].astype(F32) + s[sub(chip_id), :].astype(F32)).astype(BF16)

        fold(far_chip)
        m(M1L).start()
        m(M1R).start()
        fold(left_chip)
        m(M2L).start()
        fold(right_chip)
        m(M2R).start()
        own[slot] = p[block(chip), :].astype(F32) + s[sub(chip), :].astype(F32)

        @pl.when(g < total - 1)
        def _():
            pl.semaphore_signal(credit, inc=1, device_id={"tp": sib}, device_id_type=MESH)

    def reduce_second(g):
        slot = g % 2
        m = messages(g)
        m(M1L).wait_recv()
        m3[0] = (part[block(left_chip), first].astype(F32) + ro[slot, 0].astype(F32)).astype(BF16)
        m(M3L).start()
        m(M1R).wait_recv()
        m3[1] = (part[block(right_chip), second].astype(F32) + ro[slot, 1].astype(F32)).astype(BF16)
        m(M3R).start()

    def reduce_last(g):
        slot = g % 2
        c = g % n_chunks
        m = messages(g)
        for kind in (M2L, M2R, M3L, M3R):
            m(kind).wait_recv()

        @pl.when(g < n_chunks)
        def _():
            residual_copy(c).wait()

        h = (own[slot] + (rf[slot, 0].astype(F32) + rf[slot, 1].astype(F32)) + hres[c].astype(F32)).astype(BF16)
        hres[c] = h
        ag[g % AG_SLOTS, sub(chip), :] = h
        for kind in (A1L, A1R):
            m(kind).start()

    def gather_second(g):
        m = messages(g)
        for kind in (A2L, A2R):
            m(kind).start()

    def gather_forward(g):
        m = messages(g)
        m(A1L).wait_recv()
        m(A3L).start()
        m(A1R).wait_recv()
        m(A3R).start()

    def gather_last(g):
        slot = g % 2
        m = messages(g)
        start = gathered(g)[0]
        for kind in (A2L, A2R):
            m(kind).wait_recv()
        start((0, 1, 2), False)
        for kind in (A3L, A3R):
            m(kind).wait_recv()
        start((3,), True)

    def gather_sibling(g):
        for n in range(4):
            gathered(g)[2](y_ref, n).wait_recv()

    def gather_done(g):
        m = messages(g)
        for kind in (A1L, A1R, A2L, A2R, A3L, A3R):
            m(kind).wait_send()
        _, to_mine, to_sibling = gathered(g)
        to_mine(y_ref).wait()
        for n in range(4):
            to_sibling(y_ref, n).wait_send()

    def first_done(g):
        m = messages(g)
        for kind in (SIB, M1L, M1R, M2L, M2R):
            m(kind).wait_send()

    def second_done(g):
        m = messages(g)
        for kind in (M3L, M3R):
            m(kind).wait_send()

    def guarded(g, fn):
        @pl.when(jnp.logical_and(g >= 0, g < total))
        def _():
            fn(g)

    def normalize(g, part_idx, n_parts):
        size = rows // n_parts
        rr = pl.ds(part_idx * size, size)
        gain = ng_ref[pl.ds(jnp.minimum(g // n_chunks, n_layers - 1), 1), :]
        xn[rr, :] = norm_last(xn[rr, :].astype(F32), gain).astype(BF16)

    def expand(g):
        n = xn[...]
        layer = g // n_chunks
        here = pl.ds(seq_start(g), rows)
        for n_row in range(rows // HEAD_DIM):
            tokens_here = pl.ds(pl.multiple_of(seq_start(g) + n_row * HEAD_DIM, HEAD_DIM), HEAD_DIM)
            both = pos_ref[:, tokens_here].astype(F32)
            wanted = lax.broadcasted_iota(jnp.int32, both.shape, 0) == (g % n_chunks) // per_seq
            row = jnp.sum(jnp.where(wanted, both, 0.0), axis=0, keepdims=True)
            down = jnp.transpose(jnp.broadcast_to(row, (HEAD_DIM, HEAD_DIM)))
            cos, sin = cos_sin(down * fr_ref[0:1, :])
            part_rows = slice(n_row * HEAD_DIM, (n_row + 1) * HEAD_DIM)
            cs[part_rows, :] = cos
            sn[part_rows, :] = sin * fr_ref[1:2, :]

        def head(values, gain):
            return rope(norm_last(values, gain), cs[...], sn[...]).astype(BF16)

        def put_k(values):
            k_scr[here, :HEAD_DIM] = head(values, kg_ref[layer])

        def put_q(hd):
            def put(values):
                q_scr[hd, :, :HEAD_DIM] = head(values, qg_ref[layer, hd:hd + 1, :])
            return put

        z = mm(n, wqkv[:, qw:qw + 2 * HEAD_DIM])
        v_scr[here, :HEAD_DIM] = z[:, HEAD_DIM:].astype(BF16)
        pending = [(put_k, z[:, :HEAD_DIM])]
        row_id = seq_start(g) + lax.broadcasted_iota(jnp.int32, (rows, HEAD_DIM), 0)
        lane = lax.broadcasted_iota(jnp.int32, (rows, HEAD_DIM), 1)
        length = len_ref[(g % n_chunks) // per_seq]
        k_scr[here, HEAD_DIM:] = jnp.where(jnp.logical_and(lane == 0, row_id >= length), NEG, 0.0).astype(BF16)
        for pair in range(heads // 2):
            z = mm(n, wqkv[:, pair * 2 * HEAD_DIM:(pair + 1) * 2 * HEAD_DIM])
            pending += [(put_q(2 * pair + e), z[:, e * HEAD_DIM:(e + 1) * HEAD_DIM]) for e in range(2)]
        for c0 in range(0, ff, 256):
            c1 = min(c0 + 256, ff)
            gate = mm_t(n, wg[c0:c1, :])
            up = mm_t(n, wu[c0:c1, :])
            if pending:
                put, values = pending.pop(0)
                put(values)
            act[:, qw + c0:qw + c1] = (jax.nn.silu(gate) * up).astype(BF16)
        for put, values in pending:
            put(values)

    def attention(g):
        s0 = seq_start(g)
        lanes = HEAD_DIM
        size = min(rows, 256)

        def stream(units, scores, soft, weigh):
            following, last = scores(units[0]), None
            for n, unit in enumerate(units):
                current = following
                if n + 1 < len(units):
                    following = scores(units[n + 1])
                probs = soft(unit, current)
                if last is not None:
                    weigh(*last)
                last = (unit, probs)
            weigh(*last)

        def top_of(tiles):
            top = tiles[0]
            for t in tiles[1:]:
                top = jnp.maximum(top, t)
            return jnp.max(top, axis=-1, keepdims=True)

        def probs_of(tiles, top):
            return jnp.concatenate([jnp.exp2((t - top) * c_exp).astype(BF16) for t in tiles], axis=1)

        step = 2 * size
        n_units = rows // size
        offset = lax.broadcasted_iota(jnp.int32, (size, lanes), 0) - lax.broadcasted_iota(jnp.int32, (size, lanes), 1)

        def own(first_half):
            base = pl.multiple_of(s0 - first_half * size, size)

            def own_keys(n):
                return pl.ds(base, (first_half + n + 1) * size)

            def own_scores(unit):
                hd, n = unit
                return mm_t(q_scr[hd, n * size:(n + 1) * size, :], k_scr[own_keys(n), :])

            def own_soft(unit, s):
                hd, n = unit
                before = (first_half + n) * size
                tiles = []
                for t in range(0, before + size, lanes):
                    tile = s[:, t:t + lanes]
                    tiles.append(tile if t < before else jnp.where(offset >= t - before, tile, NEG))
                top = top_of(tiles)
                m_scr[hd, n * size:(n + 1) * size, :] = jnp.broadcast_to(top, (size, lanes))
                return probs_of(tiles, top)

            def own_weigh(unit, p):
                hd, n = unit
                acc_scr[hd, n * size:(n + 1) * size, :] = mm(p, v_scr[own_keys(n), :])

            stream([(hd, n) for hd in range(heads) for n in range(n_units)], own_scores, own_soft, own_weigh)

        if n_units == 2:
            own(0)
        else:
            for odd in range(2):
                @pl.when((s0 // size) % 2 == odd)
                def _():
                    own(odd)

        def body(j, carry):
            keys = pl.ds(pl.multiple_of(j * step, step), step)

            def scores(hd):
                return mm_t(q_scr[hd], k_scr[keys, :])

            def soft(hd, s):
                tiles = [s[:, t:t + lanes] for t in range(0, step, lanes)]
                old = m_scr[hd]
                top = jnp.maximum(old, top_of(tiles))
                m_scr[hd] = top
                return probs_of(tiles, top), jnp.exp2((old - top) * c_exp)

            def weigh(hd, probs):
                p, scale = probs
                pv = mm(p, v_scr[keys, :])
                acc_scr[hd, :, :lanes] = acc_scr[hd, :, :lanes] * scale + pv[:, :lanes]
                acc_scr[hd, :, lanes:] = acc_scr[hd, :, lanes:] * scale + pv[:, lanes:]

            stream(list(range(heads)), scores, soft, weigh)
            return carry

        lax.fori_loop(0, s0 // step, body, 0)
        for hd in range(heads):
            out = acc_scr[hd, :, :lanes] / acc_scr[hd, :, lanes:]
            act[:, hd * lanes:(hd + 1) * lanes] = out.astype(BF16)

    def output(g, side):
        p = part
        r = (sib_half, my_half)[side]
        a = act[r, :]
        n_cols = 2
        step = width // n_cols
        for n in range(n_cols):
            p[r, n * step:(n + 1) * step] = mm(a, wod[:, n * step:(n + 1) * step]).astype(BF16)
            normalize(g + 1, 2 * side + n, 4)

    def layer_start(g, which):
        @pl.when(g % n_chunks == 0)
        def _():
            for copy in weight_copies(which, g // n_chunks):
                copy.wait()

    def layer_end(g, which):
        @pl.when(jnp.logical_and(g % n_chunks == n_chunks - 1, g < total - 1))
        def _():
            for copy in weight_copies(which, g // n_chunks + 1):
                copy.start()

    start_input(0)
    for copy in weight_copies("qkv", 0) + weight_copies("ff", 0):
        copy.start()
    barrier = pltpu.get_barrier_semaphore()
    for dev in (left, right, sib):
        pl.semaphore_signal(barrier, inc=1, device_id={"tp": dev}, device_id_type=MESH)
    q_scr[:, :, HEAD_DIM:] = jnp.ones((heads, rows, HEAD_DIM), BF16)
    v_scr[:, HEAD_DIM:] = jnp.ones((v_scr.shape[0], HEAD_DIM), BF16)
    pad = act.shape[1] - (qw + ff)
    if pad:
        act[:, qw + ff:] = jnp.zeros((rows, pad), BF16)
        wod[qw + ff:, :] = jnp.zeros((pad, width), BF16)
    wait_input(0)
    for n in range(4):
        normalize(0, n, 4)
    pl.semaphore_wait(barrier, 3)

    def step(i, carry):
        busy = i < total

        @pl.when(busy)
        def _():
            layer_start(i, "qkv")
            layer_start(i, "ff")

            @pl.when(i == 0)
            def _():
                for copy in weight_copies("od", 0):
                    copy.start()
                for c in range(n_chunks):
                    residual_copy(c).start()

            expand(i)
            layer_end(i, "qkv")
            layer_end(i, "ff")
            for copy in kv_copies(i):
                copy.start()

            @pl.when(i + 1 < total)
            def _():
                start_input(i + 1)

        guarded(i - 4, gather_done)
        guarded(i - 2, second_done)
        guarded(i - 1, reduce_second)
        guarded(i - 2, gather_second)

        @pl.when(busy)
        def _():
            attention(i)
            for copy in kv_copies(i):
                copy.wait()

        guarded(i - 2, gather_forward)
        guarded(i - 3, gather_last)
        guarded(i - 1, first_done)

        @pl.when(busy)
        def _():
            layer_start(i, "od")

            @pl.when(i + 1 < total)
            def _():
                wait_input(i + 1)

            output(i, 0)

            @pl.when(i > 0)
            def _():
                pl.semaphore_wait(credit, 1)

            messages(i)(SIB).start()
            output(i, 1)
            layer_end(i, "od")

        guarded(i, reduce_first)
        guarded(i - 1, reduce_last)
        guarded(i - 3, gather_sibling)
        return carry

    lax.fori_loop(0, total + 4, step, 0)


def hand_over(*arrays):
    n_parts = (16, 2, 2)
    sizes = [a.shape[0] // n for a, n in zip(arrays, n_parts)]

    def kernel(*refs):
        n = len(arrays)
        ins, outs, bufs, sems = refs[:n], refs[n:2 * n], refs[2 * n:3 * n], refs[3 * n]
        reads, writes, count = [], [], 0
        for src, dst, buf, parts, size in zip(ins, outs, bufs, n_parts, sizes):
            for part_idx in range(parts):
                there = pl.ds(part_idx * size, size)
                reads.append(pltpu.make_async_copy(src.at[there], buf.at[part_idx], sems.at[0, count]))
                writes.append(pltpu.make_async_copy(buf.at[part_idx], dst.at[there], sems.at[1, count]))
                count += 1
        for copy in reads:
            copy.start()
        for read, write in zip(reads, writes):
            read.wait()
            write.start()
        for copy in writes:
            copy.wait()

    return pl.pallas_call(
        kernel,
        name="hand_over",
        out_shape=tuple(jax.ShapeDtypeStruct(a.shape, a.dtype) for a in arrays),
        in_specs=[pl.BlockSpec(memory_space=pl.ANY)] * len(arrays),
        out_specs=(pl.BlockSpec(memory_space=pl.ANY),) * len(arrays),
        scratch_shapes=[pltpu.VMEM((n, size) + a.shape[1:], a.dtype) for a, n, size in zip(arrays, n_parts, sizes)]
        + [pltpu.SemaphoreType.DMA((2, sum(n_parts)))],
        compiler_params=pltpu.CompilerParams(vmem_limit_bytes=60000000),
    )(*arrays)


def run_layers(x, positions, lengths, w_q, w_k, w_v, w_o, w_gate, w_up, w_down, norm_gain, q_gain, k_gain, n_tp):
    n_batch, seq, width = x.shape
    n_layers = w_q.shape[0]
    heads = w_q.shape[2] // HEAD_DIM
    ff = w_gate.shape[2]
    rows = min(CHUNK_ROWS, seq // 4)
    tokens = n_batch * seq
    n_chunks, per_seq, chips = tokens // rows, seq // rows, n_tp // 2
    quarter = rows // n_tp
    act_width = -(-(heads * HEAD_DIM + ff) // 256) * 256
    cfg = (n_layers, n_chunks, rows, per_seq, heads, chips)
    lane = np.arange(HEAD_DIM)
    freqs = np.stack([ROPE_THETA ** (-(lane // 2) * (2.0 / HEAD_DIM)), np.where(lane % 2 == 0, -1.0, 1.0)]).astype(np.float32)
    any_spec = pl.BlockSpec(memory_space=pl.ANY)
    vmem_spec = pl.BlockSpec(memory_space=pltpu.VMEM)
    dma = pltpu.SemaphoreType.DMA
    h, y, kc, vc = pl.pallas_call(
        functools.partial(layers_kernel, cfg),
        name="layers",
        out_shape=(
            jax.ShapeDtypeStruct((max(n_layers - 1, 1), tokens, width), BF16),
            jax.ShapeDtypeStruct((tokens, width), BF16),
            jax.ShapeDtypeStruct((n_layers, tokens, HEAD_DIM), BF16),
            jax.ShapeDtypeStruct((n_layers, tokens, HEAD_DIM), BF16),
        ),
        in_specs=[pl.BlockSpec(memory_space=pltpu.SMEM)] + [any_spec] * 8 + [vmem_spec] * 5,
        out_specs=(any_spec,) * 4,
        scratch_shapes=[
            pltpu.VMEM((width, (heads + 2) * HEAD_DIM), BF16),
            pltpu.VMEM((ff, width), BF16),
            pltpu.VMEM((ff, width), BF16),
            pltpu.VMEM((act_width, width), BF16),
            pltpu.VMEM((rows, width), BF16),
            pltpu.VMEM((rows, HEAD_DIM), F32),
            pltpu.VMEM((rows, HEAD_DIM), F32),
            pltpu.VMEM((rows, act_width), BF16),
            pltpu.VMEM((heads, rows, 2 * HEAD_DIM), BF16),
            pltpu.VMEM((seq, 2 * HEAD_DIM), BF16),
            pltpu.VMEM((seq, 2 * HEAD_DIM), BF16),
            pltpu.VMEM((heads, rows, HEAD_DIM), F32),
            pltpu.VMEM((heads, rows, 2 * HEAD_DIM), F32),
            pltpu.VMEM((rows, width), BF16),
            pltpu.VMEM((rows // 2, width), BF16),
            pltpu.VMEM((2, quarter, width // 2), BF16),
            pltpu.VMEM((2, quarter, width), F32),
            pltpu.VMEM((2, 2, quarter, width // 2), BF16),
            pltpu.VMEM((2, 2, quarter, width), BF16),
            pltpu.VMEM((AG_SLOTS, rows // 2, width), BF16),
            pltpu.VMEM((n_chunks, quarter, width), BF16),
            dma((7,)), dma((1,)), dma((2,)), dma((n_chunks,)), dma((AG_SLOTS,)), dma((N_MSG, AG_SLOTS)), dma((N_MSG, AG_SLOTS)),
            pltpu.SemaphoreType.REGULAR,
        ],
        compiler_params=pltpu.CompilerParams(collective_id=0, has_side_effects=True, vmem_limit_bytes=67043328),
    )(
        lengths, x.reshape(tokens, width), w_q, w_k, w_v, w_o, jnp.swapaxes(w_gate, 1, 2), jnp.swapaxes(w_up, 1, 2), w_down,
        positions, norm_gain, q_gain, k_gain, freqs
    )
    y, kc, vc = hand_over(y, kc.reshape(-1, HEAD_DIM), vc.reshape(-1, HEAD_DIM))
    y = y.reshape(n_batch, seq, width)
    cache_shape = (n_layers, n_batch, seq, 1, HEAD_DIM)
    return y, kc.reshape(cache_shape), vc.reshape(cache_shape)


def solution(mesh):
    act_spec = P('dp', None, None)
    col_spec = P(None, None, 'tp')
    row_spec = P(None, 'tp', None)
    cache_spec = P(None, 'dp', None, 'tp', None)
    in_specs = (act_spec, P('dp', None), P('dp'), col_spec, col_spec, col_spec, row_spec, col_spec, col_spec, row_spec, P(None, None), row_spec, row_spec)
    n_tp = mesh.shape['tp']

    def device_body(x, positions, lengths, w_q, w_k, w_v, w_o, w_gate, w_up, w_down, norm_gain, q_gain, k_gain):
        return run_layers(x, positions, lengths, w_q, w_k, w_v, w_o, w_gate, w_up, w_down, norm_gain, q_gain, k_gain, n_tp)

    return jax.shard_map(device_body, mesh=mesh, in_specs=in_specs, out_specs=(act_spec, cache_spec, cache_spec), check_vma=False)
```
